256 devices in a mesh: gy: 8 (over y, x_hi), gx: 32 (over x_lo, z, core).
Axes of the slice: x: 4 (x_hi: 2, x_lo: 2; x = x_hi * 2 + x_lo), y: 4, z: 8, core: 2. Of those that a mesh axis runs over, the one named last changes fastest.
Arguments:
- u_field: float32 [8, 2048, 2048], P(None, 'gx', 'gy')
- v_field: float32 [8, 2048, 2048], P(None, 'gx', 'gy')
- w_field: float32 [8, 2048, 2048], P(None, 'gx', 'gy')
- sep_x: int32 [16], replicated, may hold values from 1 to 128, as said below
- sep_y: int32 [16], replicated, may hold values from 1 to 256, as said below
- sep_z: int32 [16], replicated, may hold values from 1 to 4
Outputs:
- correlation: float32 [3, 16], replicated
The draws below stay inside these ranges and needn't reach their ends.
Inputs may be any that keep to these rules, and one draw needn't show every extreme that they name: `sep_x`: every separation along x lies in 1 to 128, and 128 is among them in every draw; repeats may occur. `sep_y`: every separation along y lies in 1 to 256, and 256 is among them in every draw; repeats may occur.
All inputs are finite; a program needn't handle non-finite values.
Results may differ from the reference program's by a relative error of at most 0.0003.
Values sent between devices are 32-bit elements; how exact they have to be, the bound alone decides.
No kernel may reach another device: no remote copies, remote signals or barrier semaphores. Data moves between devices by JAX's collectives and lax.ppermute only.
A program may use at most 64 MiB of HBM per device.

```python
import math
import jax
import jax.numpy as jnp
from jax import lax

PLANES = 8
CX = 64
CY = 256
SEPS = 16
NX = 2048
NY = 2048


def rough_scale(key, shape, spread):
    return jnp.exp(jax.random.uniform(key, shape, jnp.float32, -spread, spread))


def smooth_field(key, salt_value):
    key = jax.random.fold_in(key, salt_value)
    key_list = jax.random.split(key, 12)
    mode_count = 6
    plane_pos = jnp.arange(PLANES, dtype=jnp.float32)[:, None, None]
    row_pos = jnp.arange(NX, dtype=jnp.float32)[None, :, None]
    column_pos = jnp.arange(NY, dtype=jnp.float32)[None, None, :]
    wave_x = jax.random.randint(key_list[0], (mode_count,), 1, 5).astype(jnp.float32)
    wave_y = jax.random.randint(key_list[1], (mode_count,), 1, 5).astype(jnp.float32)
    wave_z = jax.random.randint(key_list[2], (mode_count,), 0, 3).astype(jnp.float32)
    phases = jax.random.uniform(key_list[3], (mode_count, 3), jnp.float32, 0.0, 2.0 * math.pi)
    amplitude = jax.random.uniform(key_list[4], (mode_count,), jnp.float32, 0.5, 1.0)
    smooth = jnp.zeros((PLANES, NX, NY), jnp.float32)
    for mode_index in range(mode_count):
        cos_x = jnp.cos(2.0 * math.pi * wave_x[mode_index] * row_pos / NX + phases[mode_index, 0])
        cos_y = jnp.cos(2.0 * math.pi * wave_y[mode_index] * column_pos / NY + phases[mode_index, 1])
        cos_z = jnp.cos(2.0 * math.pi * wave_z[mode_index] * plane_pos / (4.0 * PLANES) + phases[mode_index, 2])
        smooth = smooth + amplitude[mode_index] * cos_x * cos_y * cos_z
    spread = 1.15
    noise_part = 0.7 * jax.random.normal(key_list[11], (PLANES, NX, NY), jnp.float32)
    smooth_scale = rough_scale(key_list[5], (PLANES, 1, 1), spread) * rough_scale(key_list[6], (1, NX, 1), spread) * rough_scale(key_list[7], (1, 1, NY), spread)
    noise_scale = rough_scale(key_list[8], (PLANES, 1, 1), spread) * rough_scale(key_list[9], (1, NX, 1), spread) * rough_scale(key_list[10], (1, 1, NY), spread)
    return smooth_scale * (1.5 * smooth) + noise_scale * noise_part


def draw_u_field(key, part):
    return smooth_field(key, 11)


def draw_v_field(key, part):
    return smooth_field(key, 23)


def draw_w_field(key, part):
    return smooth_field(key, 37)


def separations(key, salt_value, largest):
    key = jax.random.fold_in(key, salt_value)
    key_list = jax.random.split(key, 2)
    others = jax.random.randint(key_list[0], (SEPS - 1,), 1, largest + 1)
    values = jnp.concatenate([others, jnp.full((1,), largest, jnp.int32)])
    return jax.random.permutation(key_list[1], values).astype(jnp.int32)


def draw_sep_x(key, part):
    return separations(key, 41, 2 * CX)


def draw_sep_y(key, part):
    return separations(key, 53, CY)


def touch_ends(drawn, stream_key, smallest, top_value):
    dims = drawn.shape
    index_at = [jax.random.randint(jax.random.fold_in(stream_key, axis), (), 0, dims[axis]) for axis in range(len(dims))]
    drawn = drawn.at[tuple(index_at)].set(smallest)
    longest = dims.index(max(dims))
    index_at[longest] = (index_at[longest] + 1) % dims[longest]
    return drawn.at[tuple(index_at)].set(top_value)


def setup_inputs(seed: int = 0) -> dict:
    streams_of = jax.random.split(jax.random.key(seed), 7)
    u_field = draw_u_field(jax.random.fold_in(streams_of[6], 71), 0)
    v_field = draw_v_field(jax.random.fold_in(streams_of[6], 71), 0)
    w_field = draw_w_field(jax.random.fold_in(streams_of[6], 71), 0)
    sep_x = draw_sep_x(jax.random.fold_in(streams_of[6], 71), 0)
    sep_y = draw_sep_y(jax.random.fold_in(streams_of[6], 71), 0)
    sep_z = touch_ends(jax.random.randint(streams_of[5], (SEPS,), 1, PLANES // 2 + 1), jax.random.fold_in(streams_of[5], 1), 1, (PLANES // 2 + 1) - 1).astype(jnp.int32)
    return {"u_field": u_field, "v_field": v_field, "w_field": w_field, "sep_x": sep_x, "sep_y": sep_y, "sep_z": sep_z}


def reference(u_field, v_field, w_field, sep_x, sep_y, sep_z):
    planes = u_field.shape[0]

    def along_x(lag_value):
        return jnp.sum(u_field * jnp.roll(u_field, -lag_value, axis=1))

    def along_y(lag_value):
        return jnp.sum(v_field * jnp.roll(v_field, -lag_value, axis=2))

    padded = jnp.concatenate([w_field, jnp.zeros_like(w_field)], axis=0)

    def along_z(lag_value):
        shifted = lax.dynamic_slice_in_dim(padded, lag_value.astype(jnp.int32), planes, 0)
        return jnp.sum(w_field * shifted)

    sums_x = lax.map(along_x, sep_x)
    sums_y = lax.map(along_y, sep_y)
    sums_z = lax.map(along_z, sep_z)
    energy_u = jnp.sum(u_field * u_field)
    energy_v = jnp.sum(v_field * v_field)
    energy_w = jnp.sum(w_field * w_field)
    factor = jnp.float32(planes) / (jnp.float32(planes) - sep_z.astype(jnp.float32))
    row_x = sums_x / energy_u
    row_y = sums_y / energy_v
    row_z = sums_z / energy_w * factor
    return jnp.stack([row_x, row_y, row_z], axis=0)
```

```python
import functools

import jax
import jax.numpy as jnp
from jax import lax
from jax.experimental import pallas as pl
from jax.experimental.pallas import tpu as pltpu
from jax.sharding import Mesh
from jax.sharding import PartitionSpec as P

SHAPE = (4, 2, 2, 8, 2)
AXES = ("y", "xh", "xl", "z", "c")
GX = ("xl", "z", "c")
GY = ("y", "xh")
F32 = jnp.float32
HIGH = lax.Precision.HIGHEST


def pairs_of(target):
    def flat(at):
        index = 0
        for size, i in zip(SHAPE, at):
            index = index * size + i % size
        return index

    places = [()]
    for size in SHAPE:
        places = [at + (i,) for at in places for i in range(size)]
    return [(flat(at), flat(target(*at))) for at in places]


U_KEEP = pairs_of(lambda y, xh, xl, z, c: (y, xh, xl, z - 1 + 2 * c, c))
U_SEND = pairs_of(lambda y, xh, xl, z, c: (y, xh, xl, z + 1 - 2 * c, c))
CORES = pairs_of(lambda y, xh, xl, z, c: (y, xh, xl, z, 1 - c))


def wrapped(pairs_fn):
    return pairs_of(pairs_fn)


def u_target(step):
    def target(y, xh, xl, z, c):
        chip = (xl * 8 + z + step(c)) % 16
        return (y, xh, chip // 8, chip % 8, c)

    return target


U_KEEP = pairs_of(u_target(lambda c: -1 if c == 0 else 1))
U_SEND = pairs_of(u_target(lambda c: 1 if c == 0 else -1))
V_SWAP = pairs_of(lambda y, xh, xl, z, c: (y, 1 - xh, xl, z, c))
V_KEEP = pairs_of(lambda y, xh, xl, z, c: (y - 1 if xh == 0 else y + 1, xh, xl, z, c))


def dot_nt(a, b):
    return lax.dot_general(a, b, (((1,), (1,)), ((), ())), precision=HIGH, preferred_element_type=F32)


def dot_tn(a, b):
    return lax.dot_general(a, b, (((0,), (0,)), ((), ())), precision=HIGH, preferred_element_type=F32)


def lane_index():
    return lax.broadcasted_iota(jnp.int32, (8, 128), 1)


def row_index():
    return lax.broadcasted_iota(jnp.int32, (8, 128), 0)


def lag_row(refs):
    lane = lane_index()
    lags = jnp.zeros((8, 128), jnp.int32)
    for axis, ref in enumerate(refs):
        for k in range(16):
            lags = jnp.where(lane == axis * 16 + k, ref[k], lags)
    return lags


def skewed(gram):
    rows, lanes = gram.shape
    total = gram[:8]
    for i in range(8, rows, 8):
        total = total + pltpu.roll(gram[i : i + 8], (lanes - i) % lanes, 1)
    return total


def pick(skew, diagonal):
    lanes = skew.shape[1]
    at = (diagonal + row_index()) & (lanes - 1)
    got = jnp.zeros((8, 128), F32)
    for t in range(lanes // 128):
        part = jnp.take_along_axis(skew[:, t * 128 : (t + 1) * 128], at & 127, axis=1)
        got = jnp.where((at >> 7) == t, part, got)
    return jnp.broadcast_to(jnp.sum(got, axis=0, keepdims=True), (8, 128))


def widened(gram):
    return jnp.concatenate([gram, jnp.zeros(gram.shape, F32)], axis=1)


def own_kernel(sx, sy, sz, u_ref, v_ref, w_ref, out_ref):
    lags = lag_row((sx, sy, sz))
    lane = lane_index()
    u_gram = jnp.zeros((64, 128), F32)
    pad = jnp.zeros((64, 256), F32)
    for z in range(8):
        plane = u_ref[z]
        u_gram = u_gram + dot_nt(plane, jnp.concatenate([plane, pad], axis=0))
    u_sums = pick(skewed(u_gram), lags)
    u_sums = jnp.where(lags < 64, u_sums, 0.0)
    v_rows = v_ref[...].reshape(512, 256)
    v_sums = pick(skewed(widened(dot_tn(v_rows, v_rows))), lags)
    planes = [w_ref[z] for z in range(8)]
    w_sums = jnp.zeros((8, 128), F32)
    for lag in range(5):
        total = planes[0] * planes[lag]
        for z in range(1, 8 - lag):
            total = total + planes[z] * planes[z + lag]
        total = jnp.sum(jnp.sum(total, axis=0, keepdims=True), axis=1, keepdims=True)
        w_sums = jnp.where(lags == lag, total, w_sums)
    w_sums = w_sums * 8.0 / (8.0 - lags.astype(F32))
    of_u = (lane < 16) | (lane == 48)
    of_v = (lane < 32) | (lane == 49)
    out_ref[...] = jnp.where(of_u, u_sums, jnp.where(of_v, v_sums, w_sums))


def v_kernel(sx, sy, sz, own, other, near, before, out_ref):
    lags = lag_row((sx, sy, sz))
    lane = lane_index()
    first = lax.axis_index("xh") == 0
    a = own[...].reshape(256, 256)
    b = other[...].reshape(256, 256)
    c = near[...].reshape(256, 256)
    gram = dot_tn(a, b) + dot_tn(b, c)
    sums = pick(skewed(widened(gram)), jnp.where(first, lags - 256, 256 - lags))
    out_ref[...] = before[...] + jnp.where((lane >= 16) & (lane < 32), sums, 0.0)


def u_kernel(sx, sy, sz, keep, send, other, near_keep, near_send, before, out_ref):
    lags = lag_row((sx, sy, sz))
    lane = lane_index()
    first = lax.axis_index("c") == 0
    gram = jnp.zeros((64, 128), F32)
    pad = jnp.zeros((64, 256), F32)
    for z in range(4):
        a, b, c = keep[z], other[z], near_keep[z]
        gram = gram + dot_nt(a, jnp.concatenate([b, c], axis=0))
        gram = gram + dot_nt(b, jnp.concatenate([c, pad], axis=0))
        gram = gram + dot_nt(near_send[z], jnp.concatenate([pad, send[z]], axis=0))
    i = lax.broadcasted_iota(jnp.int32, (64, 128), 0)
    j = lax.broadcasted_iota(jnp.int32, (64, 128), 1) - 64
    ahead = jnp.where(first, i - j, j - i)
    gram = jnp.where((j < 0) | (ahead >= 0), gram, 0.0)
    sums = pick(skewed(gram), jnp.where(first, lags - 64, 64 - lags))
    out_ref[...] = before[...] + jnp.where(lane < 16, sums, 0.0)


def end_kernel(parts, out_ref):
    total = parts[0]
    for d in range(1, parts.shape[0]):
        total = total + parts[d]
    lane = lax.broadcasted_iota(jnp.int32, (1, 128), 1)
    for axis in range(3):
        energy = jnp.sum(jnp.where(lane == 48 + axis, total, 0.0), axis=1, keepdims=True)
        out_ref[axis : axis + 1, :] = total[:, axis * 16 : axis * 16 + 16] / energy


SMEM = pl.BlockSpec(memory_space=pltpu.SMEM)
VMEM = pl.BlockSpec(memory_space=pltpu.VMEM)


def call(kernel, shape, *args):
    specs = [SMEM if a.dtype == jnp.int32 else VMEM for a in args]
    return pl.pallas_call(
        kernel, out_shape=jax.ShapeDtypeStruct(shape, F32), in_specs=specs, out_specs=VMEM, name=kernel.__name__
    )(*args)


def local(u, v, w, sep_x, sep_y, sep_z):
    core = lax.axis_index("c")
    half = lax.axis_index("xh")
    u_keep = lax.dynamic_slice_in_dim(u, 4 * core, 4, 0)
    u_send = lax.dynamic_slice_in_dim(u, 4 - 4 * core, 4, 0)
    v_keep = lax.dynamic_slice_in_dim(v, 4 * half, 4, 0)
    v_send = lax.dynamic_slice_in_dim(v, 4 - 4 * half, 4, 0)
    v_other = lax.ppermute(v_send, AXES, V_SWAP)
    v_near = lax.ppermute(v_keep, AXES, V_KEEP)
    near_keep = lax.ppermute(u_keep, AXES, U_KEEP)
    near_send = lax.ppermute(u_send, AXES, U_SEND)
    u_other = lax.ppermute(u_send, AXES, CORES)
    seps = (sep_x, sep_y, sep_z)
    part = call(own_kernel, (8, 128), *seps, u, v, w)
    part = call(v_kernel, (8, 128), *seps, v_keep, v_other, v_near, part)
    part = call(u_kernel, (8, 128), *seps, u_keep, u_send, u_other, near_keep, near_send, part)
    rows = lax.all_to_all(jnp.broadcast_to(part[:1], (256, 128)), AXES, 0, 0, tiled=True)
    return call(end_kernel, (3, 16), rows.reshape(256, 1, 128))


def solution(mesh):
    finer = Mesh(mesh.devices.reshape(SHAPE), AXES)
    placed = (P(None, GX, GY),) * 3 + (P(),) * 3
    return jax.shard_map(local, mesh=finer, in_specs=placed, out_specs=P(), check_vma=False)
```

```python
import jax
import jax.numpy as jnp
from jax import lax
from jax.experimental import pallas as pl
from jax.experimental.pallas import tpu as pltpu
from jax.sharding import Mesh
from jax.sharding import PartitionSpec as P


SHAPE = (4, 2, 2, 8, 2)
AXES = ("y", "xh", "xl", "z", "c")
GX = ("xl", "z", "c")
GY = ("y", "xh")
F32 = jnp.float32
HIGH = lax.Precision.HIGHEST


def pairs_of(target):
    def flat(at):
        index = 0
        for size, i in zip(SHAPE, at):
            index = index * size + i % size
        return index

    places = [()]
    for size in SHAPE:
        places = [at + (i,) for at in places for i in range(size)]
    return [(flat(at), flat(target(*at))) for at in places]


def u_target(step):
    def target(y, xh, xl, z, c):
        chip = (xl * 8 + z + step(c)) % 16
        return (y, xh, chip // 8, chip % 8, c)

    return target


U_KEEP = pairs_of(u_target(lambda c: -1 if c == 0 else 1))
U_SEND = pairs_of(u_target(lambda c: 1 if c == 0 else -1))
CORES = pairs_of(lambda y, xh, xl, z, c: (y, xh, xl, z, 1 - c))
V_SWAP = pairs_of(lambda y, xh, xl, z, c: (y, 1 - xh, xl, z, c))
V_KEEP = pairs_of(lambda y, xh, xl, z, c: (y - 1 if xh == 0 else y + 1, xh, xl, z, c))


def dot_nt(a, b):
    return lax.dot_general(a, b, (((1,), (1,)), ((), ())), precision=HIGH, preferred_element_type=F32)


def dot_tn(a, b):
    return lax.dot_general(a, b, (((0,), (0,)), ((), ())), precision=HIGH, preferred_element_type=F32)


def lane_index():
    return lax.broadcasted_iota(jnp.int32, (8, 128), 1)


def row_index():
    return lax.broadcasted_iota(jnp.int32, (8, 128), 0)


def lag_row(refs):
    lane = lane_index()
    lags = jnp.zeros((8, 128), jnp.int32)
    for axis, ref in enumerate(refs):
        for k in range(16):
            lags = jnp.where(lane == axis * 16 + k, ref[k], lags)
    return lags


def skewed(gram):
    rows, lanes = gram.shape
    total = gram[:8]
    for i in range(8, rows, 8):
        total = total + pltpu.roll(gram[i : i + 8], (lanes - i) % lanes, 1)
    return total


def pick(skew, diagonal):
    lanes = skew.shape[1]
    at = (diagonal + row_index()) & (lanes - 1)
    got = jnp.zeros((8, 128), F32)
    for t in range(lanes // 128):
        part = jnp.take_along_axis(skew[:, t * 128 : (t + 1) * 128], at & 127, axis=1)
        got = jnp.where((at >> 7) == t, part, got)
    return jnp.broadcast_to(jnp.sum(got, axis=0, keepdims=True), (8, 128))


def widened(gram):
    return jnp.concatenate([gram, jnp.zeros(gram.shape, F32)], axis=1)


def own_kernel(sx, sy, sz, u_ref, v_ref, w_ref, out_ref):
    lags = lag_row((sx, sy, sz))
    lane = lane_index()
    u_gram = jnp.zeros((64, 128), F32)
    pad = jnp.zeros((64, 256), F32)
    for z in range(8):
        plane = u_ref[z]
        u_gram = u_gram + dot_nt(plane, jnp.concatenate([plane, pad], axis=0))
    u_sums = pick(skewed(u_gram), lags)
    u_sums = jnp.where(lags < 64, u_sums, 0.0)
    v_rows = v_ref[...].reshape(512, 256)
    v_sums = pick(skewed(widened(dot_tn(v_rows, v_rows))), lags)
    planes = [w_ref[z] for z in range(8)]
    w_sums = jnp.zeros((8, 128), F32)
    for lag in range(5):
        total = planes[0] * planes[lag]
        for z in range(1, 8 - lag):
            total = total + planes[z] * planes[z + lag]
        total = jnp.sum(jnp.sum(total, axis=0, keepdims=True), axis=1, keepdims=True)
        w_sums = jnp.where(lags == lag, total, w_sums)
    w_sums = w_sums * 8.0 / (8.0 - lags.astype(F32))
    of_u = (lane < 16) | (lane == 48)
    of_v = (lane < 32) | (lane == 49)
    out_ref[...] = jnp.where(of_u, u_sums, jnp.where(of_v, v_sums, w_sums))


def swap_kernel(own, other, out_ref):
    gram = dot_tn(own[...].reshape(256, 256), other[...].reshape(256, 256))
    out_ref[...] = skewed(widened(gram))


def last_kernel(sx, sy, sz, other, near, skew, before, out_ref):
    lags = lag_row((sx, sy, sz))
    lane = lane_index()
    first = lax.axis_index("xh") == 0
    gram = dot_tn(other[...].reshape(256, 256), near[...].reshape(256, 256))
    total = skew[...] + skewed(widened(gram))
    sums = pick(total, jnp.where(first, lags - 256, 256 - lags))
    row = before[...] + jnp.where((lane >= 16) & (lane < 32), sums, 0.0)
    for i in range(0, out_ref.shape[0], 8):
        out_ref[i : i + 8] = row


def u_kernel(sx, sy, sz, keep, send, other, near_keep, near_send, before, out_ref):
    lags = lag_row((sx, sy, sz))
    lane = lane_index()
    first = lax.axis_index("c") == 0
    left = jnp.zeros((64, 128), F32)
    right = jnp.zeros((64, 64), F32)
    pad = jnp.zeros((64, 64), F32)
    for z in range(4):
        a, b, c = keep[z], other[z], near_keep[z]
        both = dot_nt(jnp.concatenate([a, b], axis=0), jnp.concatenate([b, c], axis=0))
        left = left + both[:64] + jnp.concatenate([both[64:, 64:], pad], axis=1)
        right = right + dot_nt(near_send[z], send[z])
    gram = left + jnp.concatenate([pad, right], axis=1)
    i = lax.broadcasted_iota(jnp.int32, (64, 128), 0)
    j = lax.broadcasted_iota(jnp.int32, (64, 128), 1) - 64
    ahead = jnp.where(first, i - j, j - i)
    gram = jnp.where((j < 0) | (ahead >= 0), gram, 0.0)
    sums = pick(skewed(gram), jnp.where(first, lags - 64, 64 - lags))
    out_ref[...] = before[...] + jnp.where(lane < 16, sums, 0.0)


def end_kernel(parts, out_ref):
    total = jnp.sum(parts[...], axis=0, keepdims=True)
    lane = lax.broadcasted_iota(jnp.int32, (1, 128), 1)
    for axis in range(3):
        energy = jnp.sum(jnp.where(lane == 48 + axis, total, 0.0), axis=1, keepdims=True)
        out_ref[axis : axis + 1, :] = total[:, axis * 16 : axis * 16 + 16] / energy


SMEM = pl.BlockSpec(memory_space=pltpu.SMEM)
VMEM = pl.BlockSpec(memory_space=pltpu.VMEM)


def call(kernel, out, *args):
    specs = [SMEM if a.dtype == jnp.int32 else VMEM for a in args]
    return pl.pallas_call(kernel, out_shape=out, in_specs=specs, out_specs=VMEM)(*args)


def near(x):
    return pltpu.with_memory_space_constraint(x, pltpu.VMEM)


def send(value, pairs):
    return near(lax.ppermute(value, AXES, pairs))


def local(u, v, w, sep_x, sep_y, sep_z):
    core = lax.axis_index("c")
    half = lax.axis_index("xh")
    u_keep = lax.dynamic_slice_in_dim(u, 4 * core, 4, 0)
    u_send = lax.dynamic_slice_in_dim(u, 4 - 4 * core, 4, 0)
    v_keep = lax.dynamic_slice_in_dim(v, 4 * half, 4, 0)
    v_send = lax.dynamic_slice_in_dim(v, 4 - 4 * half, 4, 0)
    v_other = send(v_send, V_SWAP)
    u_other = send(u_send, CORES)
    near_keep = send(u_keep, U_KEEP)
    near_send = send(u_send, U_SEND)
    v_near = send(v_keep, V_KEEP)
    seps = (sep_x, sep_y, sep_z)
    row = pltpu.VMEM((8, 128), F32)
    part = call(own_kernel, row, *seps, u, v, w)
    skew = call(swap_kernel, pltpu.VMEM((8, 512), F32), near(v_keep), v_other)
    part = call(u_kernel, row, *seps, near(u_keep), near(u_send), u_other, near_keep, near_send, near(part))
    rows = call(last_kernel, pltpu.VMEM((256, 128), F32), *seps, v_other, v_near, near(skew), near(part))
    rows = near(lax.all_to_all(rows, AXES, 0, 0, tiled=True))
    return call(end_kernel, jax.ShapeDtypeStruct((3, 16), F32), rows)


def solution(mesh):
    finer = Mesh(mesh.devices.reshape(SHAPE), AXES)
    placed = (P(None, GX, GY),) * 3 + (P(),) * 3
    return jax.shard_map(local, mesh=finer, in_specs=placed, out_specs=P(), check_vma=False)
```

```python
import jax
import jax.numpy as jnp
from jax import lax
from jax.experimental import pallas as pl
from jax.experimental.pallas import tpu as pltpu
from jax.sharding import Mesh
from jax.sharding import PartitionSpec as P


SHAPE = (4, 2, 2, 8, 2)
AXES = ("y", "xh", "xl", "z", "c")
GX = ("xl", "z", "c")
GY = ("y", "xh")
F32 = jnp.float32
HIGH = lax.Precision.HIGHEST


def pairs_of(target, sends=lambda *at: True):
    def flat(at):
        index = 0
        for size, i in zip(SHAPE, at):
            index = index * size + i % size
        return index

    places = [()]
    for size in SHAPE:
        places = [at + (i,) for at in places for i in range(size)]
    return [(flat(at), flat(target(*at))) for at in places if sends(*at)]


def chip_step(y, xh, xl, z, c):
    chip = xl * 8 + z + (1 if c else -1)
    return (y, xh, chip // 8, chip % 8, c)


U_CHIP = pairs_of(chip_step)
U_CORE = pairs_of(lambda y, xh, xl, z, c: (y, xh, xl, z, 1 - c))
V_HALF = pairs_of(lambda y, xh, xl, z, c: (y, c, xl, z, c), lambda y, xh, xl, z, c: xh != c)
V_NEXT = pairs_of(lambda y, xh, xl, z, c: (y + (1 if xh else -1), xh, xl, z, c), lambda y, xh, xl, z, c: xh == c)


def dot_nt(a, b):
    return lax.dot_general(a, b, (((1,), (1,)), ((), ())), precision=HIGH, preferred_element_type=F32)


def dot_tn(a, b):
    return lax.dot_general(a, b, (((0,), (0,)), ((), ())), precision=HIGH, preferred_element_type=F32)


def lane_index():
    return lax.broadcasted_iota(jnp.int32, (8, 128), 1)


def row_index():
    return lax.broadcasted_iota(jnp.int32, (8, 128), 0)


def lag_row(refs):
    lane = lane_index()
    lags = jnp.zeros((8, 128), jnp.int32)
    for axis, ref in enumerate(refs):
        for k in range(16):
            lags = jnp.where(lane == axis * 16 + k, ref[k], lags)
    return lags


def skewed(gram):
    rows, lanes = gram.shape
    total = gram[:8]
    for i in range(8, rows, 8):
        total = total + pltpu.roll(gram[i : i + 8], (lanes - i) % lanes, 1)
    return total


def pick(skew, diagonal):
    lanes = skew.shape[1]
    at = (diagonal + row_index()) & (lanes - 1)
    got = jnp.zeros((8, 128), F32)
    for t in range(lanes // 128):
        part = jnp.take_along_axis(skew[:, t * 128 : (t + 1) * 128], at & 127, axis=1)
        got = jnp.where((at >> 7) == t, part, got)
    return jnp.broadcast_to(jnp.sum(got, axis=0, keepdims=True), (8, 128))


def widened(gram):
    return jnp.concatenate([gram, jnp.zeros(gram.shape, F32)], axis=1)


def own_kernel(sx, sy, sz, u_ref, v_ref, w_ref, out_ref):
    lags = lag_row((sx, sy, sz))
    lane = lane_index()
    u_gram = jnp.zeros((64, 128), F32)
    pad = jnp.zeros((64, 256), F32)
    for z in range(8):
        plane = u_ref[z]
        u_gram = u_gram + dot_nt(plane, jnp.concatenate([plane, pad], axis=0))
    u_sums = pick(skewed(u_gram), lags)
    u_sums = jnp.where(lags < 64, u_sums, 0.0)
    v_rows = v_ref[...].reshape(512, 256)
    v_sums = pick(skewed(widened(dot_tn(v_rows, v_rows))), lags)
    planes = [w_ref[z] for z in range(8)]
    w_sums = jnp.zeros((8, 128), F32)
    for lag in range(5):
        total = planes[0] * planes[lag]
        for z in range(1, 8 - lag):
            total = total + planes[z] * planes[z + lag]
        total = jnp.sum(jnp.sum(total, axis=0, keepdims=True), axis=1, keepdims=True)
        w_sums = jnp.where(lags == lag, total, w_sums)
    w_sums = w_sums * 8.0 / (8.0 - lags.astype(F32))
    of_u = (lane < 16) | (lane == 48)
    of_v = (lane < 32) | (lane == 49)
    out_ref[...] = jnp.where(of_u, u_sums, jnp.where(of_v, v_sums, w_sums))


def v_kernel(sx, sy, sz, own, other, near, before, out_ref):
    half = lax.axis_index("xh")
    works = half == lax.axis_index("c")

    @pl.when(works)
    def _():
        lags = lag_row((sx, sy, sz))
        lane = lane_index()
        middle = other[...].reshape(512, 256)
        gram = dot_tn(own[...].reshape(512, 256), middle) + dot_tn(middle, near[...].reshape(512, 256))
        sums = pick(skewed(widened(gram)), jnp.where(half == 0, lags - 256, 256 - lags))
        out_ref[...] = before[...] + jnp.where((lane >= 16) & (lane < 32), sums, 0.0)

    @pl.when(jnp.logical_not(works))
    def _():
        out_ref[...] = before[...]


def u_kernel(sx, sy, sz, own, other, near, before, out_ref):
    lags = lag_row((sx, sy, sz))
    first = lax.axis_index("c") == 0
    grams = jnp.zeros((128, 64), F32)
    for z in range(8):
        early = jnp.where(first, own[z], near[z])
        late = jnp.where(first, near[z], own[z])
        grams = grams + dot_nt(jnp.concatenate([other[z], early], axis=0), late)
    i = lax.broadcasted_iota(jnp.int32, (64, 64), 0)
    j = lax.broadcasted_iota(jnp.int32, (64, 64), 1)
    gram = jnp.concatenate([grams[:64], jnp.where(j <= i, grams[64:], 0.0)], axis=1)
    row = before[...] + jnp.where(lane_index() < 16, pick(skewed(gram), lags - 64), 0.0)
    for i in range(0, out_ref.shape[0], 8):
        out_ref[i : i + 8] = row


def end_kernel(parts, out_ref):
    total = jnp.sum(parts[...], axis=0, keepdims=True)
    lane = lax.broadcasted_iota(jnp.int32, (1, 128), 1)
    for axis in range(3):
        energy = jnp.sum(jnp.where(lane == 48 + axis, total, 0.0), axis=1, keepdims=True)
        out_ref[axis : axis + 1, :] = total[:, axis * 16 : axis * 16 + 16] / energy


SMEM = pl.BlockSpec(memory_space=pltpu.SMEM)
VMEM = pl.BlockSpec(memory_space=pltpu.VMEM)


def call(kernel, out, *args):
    specs = [SMEM if a.dtype == jnp.int32 else VMEM for a in args]
    return pl.pallas_call(kernel, out_shape=out, in_specs=specs, out_specs=VMEM)(*args)


def near(x):
    return pltpu.with_memory_space_constraint(x, pltpu.VMEM)


def send(value, pairs):
    return near(lax.ppermute(value, AXES, pairs))


def local(u, v, w, sep_x, sep_y, sep_z):
    v_other = send(v, V_HALF)
    v_near = send(v, V_NEXT)
    u_other = send(u, U_CORE)
    u_near = send(u, U_CHIP)
    seps = (sep_x, sep_y, sep_z)
    row = pltpu.VMEM((8, 128), F32)
    part = call(own_kernel, row, *seps, u, v, w)
    part = call(v_kernel, row, *seps, v, v_other, v_near, near(part))
    rows = call(u_kernel, pltpu.VMEM((256, 128), F32), *seps, u, u_other, u_near, near(part))
    rows = near(lax.all_to_all(rows, AXES, 0, 0, tiled=True))
    return call(end_kernel, jax.ShapeDtypeStruct((3, 16), F32), rows)


def solution(mesh):
    finer = Mesh(mesh.devices.reshape(SHAPE), AXES)
    placed = (P(None, GX, GY),) * 3 + (P(),) * 3
    return jax.shard_map(local, mesh=finer, in_specs=placed, out_specs=P(), check_vma=False)
```

```python
import jax
import jax.numpy as jnp
from jax import lax
from jax.experimental import pallas as pl
from jax.experimental.pallas import tpu as pltpu
from jax.sharding import Mesh
from jax.sharding import PartitionSpec as P


SHAPE = (4, 2, 2, 8, 2)
AXES = ("y", "xh", "xl", "z", "c")
SERVED = AXES
GX = ("xl", "z", "c")
GY = ("y", "xh")
F32 = jnp.float32
BF16 = jnp.bfloat16
HIGH = lax.Precision.HIGHEST


def pairs_of(target):
    def flat(at):
        index = 0
        for size, i in zip(SHAPE, at):
            index = index * size + i % size
        return index

    places = [()]
    for size in SHAPE:
        places = [at + (i,) for at in places for i in range(size)]
    return [(flat(at), flat(target(*at))) for at in places]


def chip_step(step):
    def target(y, xh, xl, z, c):
        chip = xl * 8 + z + step[c]
        return (y, xh, chip // 8, chip % 8, c)

    return target


U_DOWN = pairs_of(chip_step((-1, -1)))
U_BOTH = pairs_of(chip_step((-1, 1)))
U_CORE = pairs_of(lambda y, xh, xl, z, c: (y, xh, xl, z, 1 - c))
V_SWAP = pairs_of(lambda y, xh, xl, z, c: (y, 1 - xh, xl, z, c))
V_NEXT = pairs_of(lambda y, xh, xl, z, c: (y + (1 if xh else -1), xh, xl, z, c))


def dot_nt(a, b, precision=HIGH):
    return lax.dot_general(a, b, (((1,), (1,)), ((), ())), precision=precision, preferred_element_type=F32)


def dot_tn(a, b):
    return lax.dot_general(a, b, (((0,), (0,)), ((), ())), precision=HIGH, preferred_element_type=F32)


def dot_nn(a, b):
    return lax.dot_general(a, b, (((1,), (0,)), ((), ())), preferred_element_type=F32)


def lane_index():
    return lax.broadcasted_iota(jnp.int32, (8, 128), 1)


def row_index():
    return lax.broadcasted_iota(jnp.int32, (8, 128), 0)


def lag_row(refs):
    lane = lane_index()
    lags = jnp.zeros((8, 128), jnp.int32)
    for axis, ref in enumerate(refs):
        for k in range(16):
            lags = jnp.where(lane == axis * 16 + k, ref[k], lags)
    return lags


def skewed(gram):
    rows, lanes = gram.shape
    total = gram[:8]
    for i in range(8, rows, 8):
        total = total + pltpu.roll(gram[i : i + 8], (lanes - i) % lanes, 1)
    return total


def pick(skew, diagonal):
    lanes = skew.shape[1]
    at = (diagonal + row_index()) & (lanes - 1)
    got = jnp.zeros((8, 128), F32)
    for t in range(lanes // 128):
        part = jnp.take_along_axis(skew[:, t * 128 : (t + 1) * 128], at & 127, axis=1)
        got = jnp.where((at >> 7) == t, part, got)
    return jnp.broadcast_to(jnp.sum(got, axis=0, keepdims=True), (8, 128))


def widened(gram):
    return jnp.concatenate([gram, jnp.zeros(gram.shape, F32)], axis=1)


def halves(x):
    high = x.astype(BF16)
    return high, (x - high.astype(F32)).astype(BF16)


def own_kernel(sx, sy, sz, u_ref, other, v_ref, w_ref, out_ref, u_parts, v_parts):
    lags = lag_row((sx, sy, sz))
    lane = lane_index()
    half = lax.axis_index("xh")
    grams = jnp.zeros((64, 128), F32)
    for z in range(8):
        a, b = u_ref[z], other[z]
        grams = grams + dot_nt(a, jnp.concatenate([a, b], axis=0))
        a_high, a_low = halves(a)
        b_high, b_low = halves(b)
        u_parts[z] = jnp.concatenate([b_high, a_high, b_low, a_low], axis=0)
    u_sums = jnp.where(lags < 64, pick(skewed(widened(grams[:, :64])), lags), 0.0)
    cores = pick(skewed(widened(grams[:, 64:])), 64 - lags)
    counted = (lax.axis_index("c") == 1) & (lags > 0) & (lags < 128)
    u_sums = u_sums + jnp.where(counted, cores, 0.0)
    keep = v_ref[pl.ds(4 * half, 4)].reshape(256, 256).T
    v_parts[:256], v_parts[256:] = halves(keep)
    v_rows = v_ref[...].reshape(512, 256)
    v_sums = pick(skewed(widened(dot_tn(v_rows, v_rows))), lags)
    planes = [w_ref[z] for z in range(8)]
    w_sums = jnp.zeros((8, 128), F32)
    for lag in range(5):
        total = planes[0] * planes[lag]
        for z in range(1, 8 - lag):
            total = total + planes[z] * planes[z + lag]
        total = jnp.sum(jnp.sum(total, axis=0, keepdims=True), axis=1, keepdims=True)
        w_sums = jnp.where(lags == lag, total, w_sums)
    w_sums = w_sums * 8.0 / (8.0 - lags.astype(F32))
    of_u = (lane < 16) | (lane == 48)
    of_v = (lane < 32) | (lane == 49)
    out_ref[...] = jnp.where(of_u, u_sums, jnp.where(of_v, v_sums, w_sums))


def u_kernel(sx, sy, sz, parts, near_down, near_both, before, out_ref):
    lags = lag_row((sx, sy, sz))
    first = lax.axis_index("c") == 0
    sums = []
    for near in (near_down, near_both):
        total = jnp.zeros((128, 64), F32)
        for i in range(4):
            z = i if near is near_down else 4 + i
            high, low = halves(near[i])
            both = dot_nt(parts[z], high, None)
            total = total + both[:128] + both[128:] + dot_nt(parts[z, :128], low, None)
        sums.append(total)
    down, mixed = sums
    far = down[64:] + jnp.where(first, mixed[64:], mixed[64:].T)
    next_to = jnp.where(first, down[:64] + mixed[:64], 0.0)
    i = lax.broadcasted_iota(jnp.int32, (64, 64), 0)
    j = lax.broadcasted_iota(jnp.int32, (64, 64), 1)
    gram = jnp.concatenate([next_to, jnp.where(j <= i, far, 0.0)], axis=1)
    out_ref[...] = before[...] + jnp.where(lane_index() < 16, pick(skewed(gram), lags - 64), 0.0)


def v_kernel(sx, sy, sz, parts, other, near, before, out_ref):
    lags = lag_row((sx, sy, sz))
    lane = lane_index()
    first = lax.axis_index("xh") == 0
    high, low = halves(other[...].reshape(256, 256))
    near_high, near_low = halves(near[...].reshape(256, 256).T)
    i = lax.broadcasted_iota(jnp.int32, (256, 256), 0)
    j = lax.broadcasted_iota(jnp.int32, (256, 256), 1)
    ahead = jnp.where(first, i - j, j - i)
    sums = jnp.zeros((8, 128), F32)
    for a_high, a_low, sign in ((parts[:256], parts[256:], 1), (near_high, near_low, -1)):
        gram = dot_nn(a_high, high) + dot_nn(a_low, high) + dot_nn(a_high, low)
        gram = jnp.where(ahead * sign >= 0, gram, 0.0)
        sums = sums + pick(skewed(gram), jnp.where(first, lags - 256, 256 - lags) * sign)
    row = before[...] + jnp.where((lane >= 16) & (lane < 32), sums, 0.0)
    for i in range(0, out_ref.shape[0], 8):
        out_ref[i : i + 8] = row


def end_kernel(parts, out_ref):
    total = jnp.sum(parts[...], axis=0, keepdims=True)
    lane = lax.broadcasted_iota(jnp.int32, (1, 128), 1)
    for axis in range(3):
        energy = jnp.sum(jnp.where(lane == 48 + axis, total, 0.0), axis=1, keepdims=True)
        out_ref[axis : axis + 1, :] = total[:, axis * 16 : axis * 16 + 16] / energy


SMEM = pl.BlockSpec(memory_space=pltpu.SMEM)
VMEM = pl.BlockSpec(memory_space=pltpu.VMEM)


def call(kernel, out, *args):
    specs = [SMEM if a.dtype == jnp.int32 else VMEM for a in args]
    return pl.pallas_call(kernel, out_shape=out, in_specs=specs, out_specs=jax.tree.map(lambda _: VMEM, out))(*args)


def near(x):
    return pltpu.with_memory_space_constraint(x, pltpu.VMEM)


def send(value, pairs):
    return near(lax.ppermute(value, AXES, pairs))


def local(u, v, w, sep_x, sep_y, sep_z):
    half = lax.axis_index("xh")
    v_keep = lax.dynamic_slice_in_dim(v, 4 * half, 4, 0)
    v_send = lax.dynamic_slice_in_dim(v, 4 - 4 * half, 4, 0)
    v_other = send(v_send, V_SWAP)
    down = send(u[:4], U_DOWN)
    both = send(u[4:], U_BOTH)
    u_other = send(u, U_CORE)
    v_near = send(v_keep, V_NEXT)
    seps = (sep_x, sep_y, sep_z)
    row = pltpu.VMEM((8, 128), F32)
    outs = (row, pltpu.VMEM((8, 256, 256), BF16), pltpu.VMEM((512, 256), BF16))
    part, u_parts, v_parts = call(own_kernel, outs, *seps, u, u_other, v, w)
    part = call(u_kernel, row, *seps, near(u_parts), down, both, near(part))
    rows = call(v_kernel, pltpu.VMEM((256, 128), F32), *seps, near(v_parts), v_other, v_near, near(part))
    rows = near(lax.all_to_all(rows, SERVED, 0, 0, tiled=True))
    return call(end_kernel, jax.ShapeDtypeStruct((3, 16), F32), rows)


def solution(mesh):
    finer = Mesh(mesh.devices.reshape(SHAPE), AXES)
    placed = (P(None, GX, GY),) * 3 + (P(),) * 3
    return jax.shard_map(local, mesh=finer, in_specs=placed, out_specs=P(), check_vma=False)
```

```python
import jax
import jax.numpy as jnp
from jax import lax
from jax.experimental import pallas as pl
from jax.experimental.pallas import tpu as pltpu
from jax.sharding import Mesh
from jax.sharding import PartitionSpec as P


SHAPE = (4, 2, 2, 8, 2)
AXES = ("y", "xh", "xl", "z", "c")
SERVED = AXES
GX = ("xl", "z", "c")
GY = ("y", "xh")
F32 = jnp.float32
UP = 3
BF16 = jnp.bfloat16
HIGH = lax.Precision.HIGHEST


def pairs_of(target):
    def flat(at):
        index = 0
        for size, i in zip(SHAPE, at):
            index = index * size + i % size
        return index

    places = [()]
    for size in SHAPE:
        places = [at + (i,) for at in places for i in range(size)]
    return [(flat(at), flat(target(*at))) for at in places]


def chip_step(step):
    def target(y, xh, xl, z, c):
        chip = xl * 8 + z + step[c]
        return (y, xh, chip // 8, chip % 8, c)

    return target


U_UP = pairs_of(chip_step((1, 1)))
U_BOTH = pairs_of(chip_step((-1, 1)))
U_CORE = pairs_of(lambda y, xh, xl, z, c: (y, xh, xl, z, 1 - c))
V_SWAP = pairs_of(lambda y, xh, xl, z, c: (y, 1 - xh, xl, z, c))
V_NEXT = pairs_of(lambda y, xh, xl, z, c: (y + (1 if xh else -1), xh, xl, z, c))


def dot_nt(a, b, precision=HIGH):
    return lax.dot_general(a, b, (((1,), (1,)), ((), ())), precision=precision, preferred_element_type=F32)


def dot_tn(a, b):
    return lax.dot_general(a, b, (((0,), (0,)), ((), ())), precision=HIGH, preferred_element_type=F32)


def dot_nn(a, b):
    return lax.dot_general(a, b, (((1,), (0,)), ((), ())), preferred_element_type=F32)


def lane_index():
    return lax.broadcasted_iota(jnp.int32, (8, 128), 1)


def row_index():
    return lax.broadcasted_iota(jnp.int32, (8, 128), 0)


def lag_row(refs):
    lane = lane_index()
    lags = jnp.zeros((8, 128), jnp.int32)
    for axis, ref in enumerate(refs):
        for k in range(16):
            lags = jnp.where(lane == axis * 16 + k, ref[k], lags)
    return lags


def skewed(gram):
    rows, lanes = gram.shape
    total = gram[:8]
    for i in range(8, rows, 8):
        total = total + pltpu.roll(gram[i : i + 8], (lanes - i) % lanes, 1)
    return total


def pick(skew, diagonal):
    lanes = skew.shape[1]
    at = (diagonal + row_index()) & (lanes - 1)
    got = jnp.zeros((8, 128), F32)
    for t in range(lanes // 128):
        part = jnp.take_along_axis(skew[:, t * 128 : (t + 1) * 128], at & 127, axis=1)
        got = jnp.where((at >> 7) == t, part, got)
    return jnp.broadcast_to(jnp.sum(got, axis=0, keepdims=True), (8, 128))


def widened(gram):
    return jnp.concatenate([gram, jnp.zeros(gram.shape, F32)], axis=1)


def halves(x):
    high = x.astype(BF16)
    return high, (x - high.astype(F32)).astype(BF16)


def split_kernel(u_ref, v_ref, up, both, keep, swap, sems):
    half = lax.axis_index("xh")
    moves = (
        (v_ref.at[pl.ds(4 - 4 * half, 4)], swap),
        (u_ref.at[pl.ds(0, UP)], up),
        (u_ref.at[pl.ds(UP, 8 - UP)], both),
        (v_ref.at[pl.ds(4 * half, 4)], keep),
    )
    copies = [pltpu.make_async_copy(a, b, sems.at[i]) for i, (a, b) in enumerate(moves)]
    for copy in copies:
        copy.start()
    for copy in copies:
        copy.wait()


def own_kernel(sx, sy, sz, u_ref, other, v_ref, w_ref, lag_ref, out_ref, u_parts, v_parts):
    lags = lag_row((sx, sy, sz))
    lag_ref[...] = lags
    lane = lane_index()
    half = lax.axis_index("xh")
    grams = jnp.zeros((64, 128), F32)
    for z in range(8):
        a, b = u_ref[z], other[z]
        grams = grams + dot_nt(a, jnp.concatenate([a, b], axis=0))
        a_high, a_low = halves(a)
        b_high, b_low = halves(b)
        u_parts[z] = jnp.concatenate([b_high, a_high, b_low, a_low], axis=0)
    u_sums = jnp.where(lags < 64, pick(skewed(widened(grams[:, :64])), lags), 0.0)
    cores = pick(skewed(widened(grams[:, 64:])), 64 - lags)
    counted = (lax.axis_index("c") == 1) & (lags > 0) & (lags < 128)
    u_sums = u_sums + jnp.where(counted, cores, 0.0)
    keep = v_ref[pl.ds(4 * half, 4)].reshape(256, 256).T
    v_parts[:256], v_parts[256:] = halves(keep)
    v_rows = v_ref[...].reshape(512, 256)
    v_sums = pick(skewed(widened(dot_tn(v_rows, v_rows))), lags)
    planes = [w_ref[z] for z in range(8)]
    w_sums = jnp.zeros((8, 128), F32)
    for lag in range(5):
        total = planes[0] * planes[lag]
        for z in range(1, 8 - lag):
            total = total + planes[z] * planes[z + lag]
        total = jnp.sum(jnp.sum(total, axis=0, keepdims=True), axis=1, keepdims=True)
        w_sums = jnp.where(lags == lag, total, w_sums)
    w_sums = w_sums * 8.0 / (8.0 - lags.astype(F32))
    of_u = (lane < 16) | (lane == 48)
    of_v = (lane < 32) | (lane == 49)
    out_ref[...] = jnp.where(of_u, u_sums, jnp.where(of_v, v_sums, w_sums))


def u_kernel(lag_ref, parts, near_up, near_both, before, out_ref):
    lags = lag_ref[...]
    first = lax.axis_index("c") == 0
    sums = []
    for near, planes in ((near_up, range(UP)), (near_both, range(UP, 8))):
        total = jnp.zeros((128, 64), F32)
        for z in planes:
            high, low = halves(near[z - planes[0]])
            both = dot_nt(parts[z], high, None)
            total = total + both[:128] + both[128:] + dot_nt(parts[z, :128], low, None)
        sums.append(total)
    up, mixed = sums
    far = jnp.where(first, mixed[64:] + up[64:].T, (mixed[64:] + up[64:]).T)
    next_to = jnp.where(first, mixed[:64], up[:64].T)
    i = lax.broadcasted_iota(jnp.int32, (64, 64), 0)
    j = lax.broadcasted_iota(jnp.int32, (64, 64), 1)
    gram = jnp.concatenate([next_to, jnp.where(j <= i, far, 0.0)], axis=1)
    out_ref[...] = before[...] + jnp.where(lane_index() < 16, pick(skewed(gram), lags - 64), 0.0)


def v_kernel(lag_ref, parts, other, near, before, out_ref):
    lags = lag_ref[...]
    lane = lane_index()
    first = lax.axis_index("xh") == 0
    high, low = halves(other[...].reshape(256, 256))
    near_high, near_low = halves(near[...].reshape(256, 256).T)
    i = lax.broadcasted_iota(jnp.int32, (256, 256), 0)
    j = lax.broadcasted_iota(jnp.int32, (256, 256), 1)
    ahead = jnp.where(first, i - j, j - i)
    sums = jnp.zeros((8, 128), F32)
    for a_high, a_low, sign in ((parts[:256], parts[256:], 1), (near_high, near_low, -1)):
        gram = dot_nn(a_high, high) + dot_nn(a_low, high) + dot_nn(a_high, low)
        gram = jnp.where(ahead * sign >= 0, gram, 0.0)
        sums = sums + pick(skewed(gram), jnp.where(first, lags - 256, 256 - lags) * sign)
    row = before[...] + jnp.where((lane >= 16) & (lane < 32), sums, 0.0)
    for i in range(0, out_ref.shape[0], 8):
        out_ref[i : i + 8] = row


def end_kernel(parts, out_ref):
    total = jnp.sum(parts[...], axis=0, keepdims=True)
    lane = lax.broadcasted_iota(jnp.int32, (1, 128), 1)
    for axis in range(3):
        energy = jnp.sum(jnp.where(lane == 48 + axis, total, 0.0), axis=1, keepdims=True)
        out_ref[axis : axis + 1, :] = total[:, axis * 16 : axis * 16 + 16] / energy


ROOM = {split_kernel: 2, own_kernel: 16, u_kernel: 12, v_kernel: 12, end_kernel: 4}
SMEM = pl.BlockSpec(memory_space=pltpu.SMEM)
VMEM = pl.BlockSpec(memory_space=pltpu.VMEM)


def call(kernel, out, *args, places=None, **more):
    places = places or [SMEM if a.dtype == jnp.int32 and a.ndim == 1 else VMEM for a in args]
    specs = jax.tree.map(lambda _: VMEM, out)
    room = pltpu.CompilerParams(vmem_limit_bytes=ROOM[kernel] * 2**20)
    return pl.pallas_call(kernel, out_shape=out, in_specs=places, out_specs=specs, compiler_params=room, **more)(*args)


def near(x):
    return pltpu.with_memory_space_constraint(x, pltpu.VMEM)


def far(x):
    return pltpu.with_memory_space_constraint(x, pltpu.HBM)


def send(value, pairs):
    return near(lax.ppermute(value, AXES, pairs))


def local(u, v, w, sep_x, sep_y, sep_z):
    pieces = [pltpu.VMEM((n, 64, 256), F32) for n in (UP, 8 - UP, 4, 4)]
    hbm = pl.BlockSpec(memory_space=pltpu.HBM)
    sems = [pltpu.SemaphoreType.DMA((4,))]
    made = call(split_kernel, pieces, far(u), far(v), places=[hbm, hbm], scratch_shapes=sems)
    u_up, u_both, v_keep, v_send = made
    v_other = send(v_send, V_SWAP)
    up = send(u_up, U_UP)
    both = send(u_both, U_BOTH)
    u_other = send(u, U_CORE)
    v_near = send(v_keep, V_NEXT)
    row = pltpu.VMEM((8, 128), F32)
    outs = (pltpu.VMEM((8, 128), jnp.int32), row, pltpu.VMEM((8, 256, 256), BF16), pltpu.VMEM((512, 256), BF16))
    made = call(own_kernel, outs, sep_x, sep_y, sep_z, u, u_other, v, w)
    lags, part, u_parts, v_parts = map(near, made)
    part = call(u_kernel, row, lags, u_parts, up, both, part)
    rows = call(v_kernel, pltpu.VMEM((256, 128), F32), lags, v_parts, v_other, v_near, near(part))
    rows = near(lax.all_to_all(rows, SERVED, 0, 0, tiled=True))
    return call(end_kernel, jax.ShapeDtypeStruct((3, 16), F32), rows)


def solution(mesh):
    finer = Mesh(mesh.devices.reshape(SHAPE), AXES)
    placed = (P(None, GX, GY),) * 3 + (P(),) * 3
    return jax.shard_map(local, mesh=finer, in_specs=placed, out_specs=P(), check_vma=False)
```

```python
import jax
import jax.numpy as jnp
from jax import lax
from jax.experimental import pallas as pl
from jax.experimental.pallas import tpu as pltpu
from jax.sharding import Mesh
from jax.sharding import PartitionSpec as P


SHAPE = (4, 2, 2, 8, 2)
AXES = ("y", "xh", "xl", "z", "c")
SERVED = AXES
GX = ("xl", "z", "c")
GY = ("y", "xh")
F32 = jnp.float32
UP = 3
BF16 = jnp.bfloat16
HIGH = lax.Precision.HIGHEST


def pairs_of(target):
    def flat(at):
        index = 0
        for size, i in zip(SHAPE, at):
            index = index * size + i % size
        return index

    places = [()]
    for size in SHAPE:
        places = [at + (i,) for at in places for i in range(size)]
    return [(flat(at), flat(target(*at))) for at in places]


def chip_step(step):
    def target(y, xh, xl, z, c):
        chip = xl * 8 + z + step[c]
        return (y, xh, chip // 8, chip % 8, c)

    return target


U_UP = pairs_of(chip_step((1, 1)))
U_BOTH = pairs_of(chip_step((-1, 1)))
U_CORE = pairs_of(lambda y, xh, xl, z, c: (y, xh, xl, z, 1 - c))
V_SWAP = pairs_of(lambda y, xh, xl, z, c: (y, 1 - xh, xl, z, c))
V_NEXT = pairs_of(lambda y, xh, xl, z, c: (y + (1 if xh else -1), xh, xl, z, c))


def dot_nt(a, b, precision=HIGH):
    return lax.dot_general(a, b, (((1,), (1,)), ((), ())), precision=precision, preferred_element_type=F32)


def dot_tn(a, b):
    return lax.dot_general(a, b, (((0,), (0,)), ((), ())), precision=HIGH, preferred_element_type=F32)


def dot_nn(a, b):
    return lax.dot_general(a, b, (((1,), (0,)), ((), ())), preferred_element_type=F32)


def lane_index():
    return lax.broadcasted_iota(jnp.int32, (8, 128), 1)


def row_index():
    return lax.broadcasted_iota(jnp.int32, (8, 128), 0)


def lag_row(refs):
    lane = lane_index()
    lags = jnp.zeros((8, 128), jnp.int32)
    for axis, ref in enumerate(refs):
        for k in range(16):
            lags = jnp.where(lane == axis * 16 + k, ref[k], lags)
    return lags


def skewed(gram):
    rows, lanes = gram.shape
    total = gram[:8]
    for i in range(8, rows, 8):
        total = total + pltpu.roll(gram[i : i + 8], (lanes - i) % lanes, 1)
    return total


def pick(skew, diagonal):
    lanes = skew.shape[1]
    at = (diagonal + row_index()) & (lanes - 1)
    got = jnp.zeros((8, 128), F32)
    for t in range(lanes // 128):
        part = jnp.take_along_axis(skew[:, t * 128 : (t + 1) * 128], at & 127, axis=1)
        got = jnp.where((at >> 7) == t, part, got)
    return jnp.broadcast_to(jnp.sum(got, axis=0, keepdims=True), (8, 128))


def widened(gram):
    return jnp.concatenate([gram, jnp.zeros(gram.shape, F32)], axis=1)


def halves(x):
    high = x.astype(BF16)
    return high, (x - high.astype(F32)).astype(BF16)


def split_kernel(u_ref, v_ref, up, both, keep, swap, sems):
    half = lax.axis_index("xh")
    moves = (
        (v_ref.at[pl.ds(4 - 4 * half, 4)], swap),
        (u_ref.at[pl.ds(0, UP)], up),
        (u_ref.at[pl.ds(UP, 8 - UP)], both),
        (v_ref.at[pl.ds(4 * half, 4)], keep),
    )
    copies = [pltpu.make_async_copy(a, b, sems.at[i]) for i, (a, b) in enumerate(moves)]
    for copy in copies:
        copy.start()
    for copy in copies:
        copy.wait()


def own_kernel(sx, sy, sz, u_up, u_both, keep, swap, w_far, lag_ref, out_ref, v_parts, w_ref, sem):
    fetch = pltpu.make_async_copy(w_far, w_ref, sem)
    fetch.start()
    lags = lag_row((sx, sy, sz))
    lag_ref[...] = lags
    lane = lane_index()
    gram = jnp.zeros((64, 128), F32)
    pad = jnp.zeros((64, 256), F32)
    for piece in (u_up, u_both):
        for z in range(piece.shape[0]):
            gram = gram + dot_nt(piece[z], jnp.concatenate([piece[z], pad], axis=0))
    u_sums = jnp.where(lags < 64, pick(skewed(gram), lags), 0.0)
    kept = keep[...].reshape(256, 256)
    sent = swap[...].reshape(256, 256)
    v_parts[:256], v_parts[256:] = halves(kept.T)
    v_sums = pick(skewed(widened(dot_tn(kept, kept) + dot_tn(sent, sent))), lags)
    fetch.wait()
    planes = [w_ref[z] for z in range(8)]
    w_sums = jnp.zeros((8, 128), F32)
    for lag in range(5):
        total = planes[0] * planes[lag]
        for z in range(1, 8 - lag):
            total = total + planes[z] * planes[z + lag]
        total = jnp.sum(jnp.sum(total, axis=0, keepdims=True), axis=1, keepdims=True)
        w_sums = jnp.where(lags == lag, total, w_sums)
    w_sums = w_sums * 8.0 / (8.0 - lags.astype(F32))
    of_u = (lane < 16) | (lane == 48)
    of_v = (lane < 32) | (lane == 49)
    out_ref[...] = jnp.where(of_u, u_sums, jnp.where(of_v, v_sums, w_sums))


def core_kernel(lag_ref, u_up, u_both, other_up, other_both, before, out_ref, u_parts):
    lags = lag_ref[...]
    gram = jnp.zeros((64, 64), F32)
    for z in range(8):
        a_high, a_low = halves(u_up[z] if z < UP else u_both[z - UP])
        b_high, b_low = halves(other_up[z] if z < UP else other_both[z - UP])
        u_parts[z] = jnp.concatenate([b_high, a_high, b_low, a_low], axis=0)
        gram = gram + dot_nt(b_high, a_high, None) + dot_nt(b_low, a_high, None) + dot_nt(b_high, a_low, None)
    counted = (lax.axis_index("c") == 1) & (lane_index() < 16) & (lags < 128)
    out_ref[...] = before[...] + jnp.where(counted, pick(skewed(widened(gram)), lags - 64), 0.0)


def u_kernel(lag_ref, parts, near_up, near_both, before, out_ref):
    lags = lag_ref[...]
    first = lax.axis_index("c") == 0
    sums = []
    for near, planes in ((near_up, range(UP)), (near_both, range(UP, 8))):
        total = jnp.zeros((128, 64), F32)
        for z in planes:
            high, low = halves(near[z - planes[0]])
            both = dot_nt(parts[z], high, None)
            total = total + both[:128] + both[128:] + dot_nt(parts[z, :128], low, None)
        sums.append(total)
    up, mixed = sums
    far = jnp.where(first, mixed[64:] + up[64:].T, (mixed[64:] + up[64:]).T)
    next_to = jnp.where(first, mixed[:64], up[:64].T)
    i = lax.broadcasted_iota(jnp.int32, (64, 64), 0)
    j = lax.broadcasted_iota(jnp.int32, (64, 64), 1)
    gram = jnp.concatenate([next_to, jnp.where(j <= i, far, 0.0)], axis=1)
    out_ref[...] = before[...] + jnp.where(lane_index() < 16, pick(skewed(gram), lags - 64), 0.0)


def v_kernel(lag_ref, parts, other, near, before, out_ref):
    lags = lag_ref[...]
    lane = lane_index()
    first = lax.axis_index("xh") == 0
    high, low = halves(other[...].reshape(256, 256))
    near_high, near_low = halves(near[...].reshape(256, 256).T)
    i = lax.broadcasted_iota(jnp.int32, (256, 256), 0)
    j = lax.broadcasted_iota(jnp.int32, (256, 256), 1)
    ahead = jnp.where(first, i - j, j - i)
    sums = jnp.zeros((8, 128), F32)
    for a_high, a_low, sign in ((parts[:256], parts[256:], 1), (near_high, near_low, -1)):
        gram = dot_nn(a_high, high) + dot_nn(a_low, high) + dot_nn(a_high, low)
        gram = jnp.where(ahead * sign >= 0, gram, 0.0)
        sums = sums + pick(skewed(gram), jnp.where(first, lags - 256, 256 - lags) * sign)
    row = before[...] + jnp.where((lane >= 16) & (lane < 32), sums, 0.0)
    for i in range(0, out_ref.shape[0], 8):
        out_ref[i : i + 8] = row


def end_kernel(parts, out_ref):
    total = jnp.sum(parts[...], axis=0, keepdims=True)
    lane = lax.broadcasted_iota(jnp.int32, (1, 128), 1)
    for axis in range(3):
        energy = jnp.sum(jnp.where(lane == 48 + axis, total, 0.0), axis=1, keepdims=True)
        out_ref[axis : axis + 1, :] = total[:, axis * 16 : axis * 16 + 16] / energy


ROOM = {core_kernel: 12, split_kernel: 2, own_kernel: 16, u_kernel: 12, v_kernel: 12, end_kernel: 4}
SMEM = pl.BlockSpec(memory_space=pltpu.SMEM)
VMEM = pl.BlockSpec(memory_space=pltpu.VMEM)


def call(kernel, out, *args, places=None, **more):
    places = places or [SMEM if a.dtype == jnp.int32 and a.ndim == 1 else VMEM for a in args]
    specs = jax.tree.map(lambda _: VMEM, out)
    room = pltpu.CompilerParams(vmem_limit_bytes=ROOM[kernel] * 2**20)
    return pl.pallas_call(kernel, out_shape=out, in_specs=places, out_specs=specs, compiler_params=room, **more)(*args)


def near(x):
    return pltpu.with_memory_space_constraint(x, pltpu.VMEM)


def far(x):
    return pltpu.with_memory_space_constraint(x, pltpu.HBM)


def send(value, pairs):
    return near(lax.ppermute(value, AXES, pairs))


def local(u, v, w, sep_x, sep_y, sep_z):
    pieces = [pltpu.VMEM((n, 64, 256), F32) for n in (UP, 8 - UP, 4, 4)]
    hbm = pl.BlockSpec(memory_space=pltpu.HBM)
    sems = [pltpu.SemaphoreType.DMA((4,))]
    made = call(split_kernel, pieces, far(u), far(v), places=[hbm, hbm], scratch_shapes=sems)
    u_up, u_both, v_keep, v_send = made
    v_other = send(v_send, V_SWAP)
    up = send(u_up, U_UP)
    both = send(u_both, U_BOTH)
    other_up = send(u_up, U_CORE)
    other_both = send(u_both, U_CORE)
    v_near = send(v_keep, V_NEXT)
    row = pltpu.VMEM((8, 128), F32)
    outs = (pltpu.VMEM((8, 128), jnp.int32), row, pltpu.VMEM((512, 256), BF16))
    args = (sep_x, sep_y, sep_z, *map(near, (u_up, u_both, v_keep, v_send)), far(w))
    places = [SMEM] * 3 + [VMEM] * 4 + [hbm]
    scratch = [pltpu.VMEM((8, 64, 256), F32), pltpu.SemaphoreType.DMA]
    lags, part, v_parts = map(near, call(own_kernel, outs, *args, places=places, scratch_shapes=scratch))
    outs = (row, pltpu.VMEM((8, 256, 256), BF16))
    part, u_parts = map(near, call(core_kernel, outs, lags, near(u_up), near(u_both), other_up, other_both, part))
    part = call(u_kernel, row, lags, u_parts, up, both, part)
    rows = call(v_kernel, pltpu.VMEM((256, 128), F32), lags, v_parts, v_other, v_near, near(part))
    rows = near(lax.all_to_all(rows, SERVED, 0, 0, tiled=True))
    return call(end_kernel, jax.ShapeDtypeStruct((3, 16), F32), rows)


def solution(mesh):
    finer = Mesh(mesh.devices.reshape(SHAPE), AXES)
    placed = (P(None, GX, GY),) * 3 + (P(),) * 3
    return jax.shard_map(local, mesh=finer, in_specs=placed, out_specs=P(), check_vma=False)
```

```python
import jax
import jax.numpy as jnp
from jax import lax
from jax.experimental import pallas as pl
from jax.experimental.pallas import tpu as pltpu
from jax.sharding import Mesh
from jax.sharding import PartitionSpec as P


SHAPE = (4, 2, 2, 8, 2)
AXES = ("y", "xh", "xl", "z", "c")
SERVED = AXES
GX = ("xl", "z", "c")
GY = ("y", "xh")
F32 = jnp.float32
UP = 3
BF16 = jnp.bfloat16


def pairs_of(target):
    def flat(at):
        index = 0
        for size, i in zip(SHAPE, at):
            index = index * size + i % size
        return index

    places = [()]
    for size in SHAPE:
        places = [at + (i,) for at in places for i in range(size)]
    return [(flat(at), flat(target(*at))) for at in places]


def chip_step(step):
    def target(y, xh, xl, z, c):
        chip = xl * 8 + z + step[c]
        return (y, xh, chip // 8, chip % 8, c)

    return target


U_UP = pairs_of(chip_step((1, 1)))
U_BOTH = pairs_of(chip_step((-1, 1)))
U_CORE = pairs_of(lambda y, xh, xl, z, c: (y, xh, xl, z, 1 - c))
V_SWAP = pairs_of(lambda y, xh, xl, z, c: (y, 1 - xh, xl, z, c))
V_NEXT = pairs_of(lambda y, xh, xl, z, c: (y + (1 if xh else -1), xh, xl, z, c))


def dot_nt(a, b):
    return lax.dot_general(a, b, (((1,), (1,)), ((), ())), preferred_element_type=F32)


def dot_nn(a, b):
    return lax.dot_general(a, b, (((1,), (0,)), ((), ())), preferred_element_type=F32)


def lane_index():
    return lax.broadcasted_iota(jnp.int32, (8, 128), 1)


def row_index():
    return lax.broadcasted_iota(jnp.int32, (8, 128), 0)


def lag_row(refs):
    lane = lane_index()
    lags = jnp.zeros((8, 128), jnp.int32)
    for axis, ref in enumerate(refs):
        for k in range(16):
            lags = jnp.where(lane == axis * 16 + k, ref[k], lags)
    return lags


def skewed(gram):
    rows, lanes = gram.shape
    total = gram[:8]
    for i in range(8, rows, 8):
        total = total + pltpu.roll(gram[i : i + 8], (lanes - i) % lanes, 1)
    return total


def pick(skew, diagonal):
    lanes = skew.shape[1]
    at = (diagonal + row_index()) & (lanes - 1)
    got = jnp.zeros((8, 128), F32)
    for t in range(lanes // 128):
        part = jnp.take_along_axis(skew[:, t * 128 : (t + 1) * 128], at & 127, axis=1)
        got = jnp.where((at >> 7) == t, part, got)
    return jnp.broadcast_to(jnp.sum(got, axis=0, keepdims=True), (8, 128))


def widened(gram):
    return jnp.concatenate([gram, jnp.zeros(gram.shape, F32)], axis=1)


def halves(x):
    high = x.astype(BF16)
    return high, (x - high.astype(F32)).astype(BF16)


def split_kernel(u_ref, v_ref, up, both, keep, swap, sems):
    half = lax.axis_index("xh")
    moves = (
        (v_ref.at[pl.ds(4 - 4 * half, 4)], swap),
        (u_ref.at[pl.ds(0, UP)], up),
        (u_ref.at[pl.ds(UP, 8 - UP)], both),
        (v_ref.at[pl.ds(4 * half, 4)], keep),
    )
    copies = [pltpu.make_async_copy(a, b, sems.at[i]) for i, (a, b) in enumerate(moves)]
    for copy in copies:
        copy.start()
    for copy in copies:
        copy.wait()


def own_kernel(sx, sy, sz, u_up, u_both, keep, swap, w_far, lag_ref, out_ref, v_parts, w_ref, sem):
    fetch = pltpu.make_async_copy(w_far, w_ref, sem)
    fetch.start()
    lags = lag_row((sx, sy, sz))
    lag_ref[...] = lags
    lane = lane_index()
    gram = jnp.zeros((64, 64), F32)
    for piece in (u_up, u_both):
        for z in range(piece.shape[0]):
            high, low = halves(piece[z])
            both = dot_nt(jnp.concatenate([high, low], axis=0), high)
            gram = gram + both[:64] + both[64:] + dot_nt(high, low)
    u_sums = jnp.where(lags < 64, pick(skewed(widened(gram)), lags), 0.0)
    gram = jnp.zeros((256, 256), F32)
    for piece in (keep, swap):
        rows = piece[...].reshape(256, 256)
        high, low = halves(rows)
        t_high, t_low = halves(rows.T)
        gram = gram + dot_nn(t_high, high) + dot_nn(t_low, high) + dot_nn(t_high, low)
        if piece is keep:
            v_parts[:256] = t_high
            v_parts[256:] = t_low
    v_sums = pick(skewed(widened(gram)), lags)
    fetch.wait()
    planes = [w_ref[z] for z in range(8)]
    w_sums = jnp.zeros((8, 128), F32)
    for lag in range(5):
        total = planes[0] * planes[lag]
        for z in range(1, 8 - lag):
            total = total + planes[z] * planes[z + lag]
        total = jnp.sum(jnp.sum(total, axis=0, keepdims=True), axis=1, keepdims=True)
        w_sums = jnp.where(lags == lag, total, w_sums)
    w_sums = w_sums * 8.0 / (8.0 - lags.astype(F32))
    of_u = (lane < 16) | (lane == 48)
    of_v = (lane < 32) | (lane == 49)
    out_ref[...] = jnp.where(of_u, u_sums, jnp.where(of_v, v_sums, w_sums))


def core_kernel(lag_ref, u_up, u_both, other_up, other_both, before, out_ref, u_parts):
    lags = lag_ref[...]
    gram = jnp.zeros((64, 64), F32)
    for z in range(8):
        a_high, a_low = halves(u_up[z] if z < UP else u_both[z - UP])
        b_high, b_low = halves(other_up[z] if z < UP else other_both[z - UP])
        u_parts[z] = jnp.concatenate([b_high, a_high, b_low, a_low], axis=0)
        gram = gram + dot_nt(b_high, a_high) + dot_nt(b_low, a_high) + dot_nt(b_high, a_low)
    counted = (lax.axis_index("c") == 1) & (lane_index() < 16) & (lags < 128)
    out_ref[...] = before[...] + jnp.where(counted, pick(skewed(widened(gram)), lags - 64), 0.0)


def u_kernel(lag_ref, parts, near_up, near_both, before, out_ref):
    lags = lag_ref[...]
    first = lax.axis_index("c") == 0
    sums = []
    for near, planes in ((near_up, range(UP)), (near_both, range(UP, 8))):
        total = jnp.zeros((128, 64), F32)
        for z in planes:
            high, low = halves(near[z - planes[0]])
            both = dot_nt(parts[z], high)
            total = total + both[:128] + both[128:] + dot_nt(parts[z, :128], low)
        sums.append(total)
    up, mixed = sums
    far = jnp.where(first, mixed[64:] + up[64:].T, (mixed[64:] + up[64:]).T)
    next_to = jnp.where(first, mixed[:64], up[:64].T)
    i = lax.broadcasted_iota(jnp.int32, (64, 64), 0)
    j = lax.broadcasted_iota(jnp.int32, (64, 64), 1)
    gram = jnp.concatenate([next_to, jnp.where(j <= i, far, 0.0)], axis=1)
    out_ref[...] = before[...] + jnp.where(lane_index() < 16, pick(skewed(gram), lags - 64), 0.0)


def v_kernel(lag_ref, parts, other, near, before, out_ref):
    lags = lag_ref[...]
    lane = lane_index()
    first = lax.axis_index("xh") == 0
    high, low = halves(other[...].reshape(256, 256))
    near_high, near_low = halves(near[...].reshape(256, 256).T)
    i = lax.broadcasted_iota(jnp.int32, (256, 256), 0)
    j = lax.broadcasted_iota(jnp.int32, (256, 256), 1)
    ahead = jnp.where(first, i - j, j - i)
    sums = jnp.zeros((8, 128), F32)
    for a_high, a_low, sign in ((parts[:256], parts[256:], 1), (near_high, near_low, -1)):
        gram = dot_nn(a_high, high) + dot_nn(a_low, high) + dot_nn(a_high, low)
        gram = jnp.where(ahead * sign >= 0, gram, 0.0)
        sums = sums + pick(skewed(gram), jnp.where(first, lags - 256, 256 - lags) * sign)
    row = before[...] + jnp.where((lane >= 16) & (lane < 32), sums, 0.0)
    for i in range(0, out_ref.shape[0], 8):
        out_ref[i : i + 8] = row


def end_kernel(parts, out_ref):
    total = jnp.sum(parts[...], axis=0, keepdims=True)
    lane = lax.broadcasted_iota(jnp.int32, (1, 128), 1)
    for axis in range(3):
        energy = jnp.sum(jnp.where(lane == 48 + axis, total, 0.0), axis=1, keepdims=True)
        out_ref[axis : axis + 1, :] = total[:, axis * 16 : axis * 16 + 16] / energy


ROOM = {core_kernel: 12, split_kernel: 2, own_kernel: 16, u_kernel: 12, v_kernel: 12, end_kernel: 4}
SMEM = pl.BlockSpec(memory_space=pltpu.SMEM)
VMEM = pl.BlockSpec(memory_space=pltpu.VMEM)


def call(kernel, out, *args, places=None, **more):
    places = places or [SMEM if a.dtype == jnp.int32 and a.ndim == 1 else VMEM for a in args]
    specs = jax.tree.map(lambda _: VMEM, out)
    room = pltpu.CompilerParams(vmem_limit_bytes=ROOM[kernel] * 2**20)
    return pl.pallas_call(kernel, out_shape=out, in_specs=places, out_specs=specs, compiler_params=room, **more)(*args)


def near(x):
    return pltpu.with_memory_space_constraint(x, pltpu.VMEM)


def far(x):
    return pltpu.with_memory_space_constraint(x, pltpu.HBM)


def send(value, pairs):
    return near(lax.ppermute(value, AXES, pairs))


def local(u, v, w, sep_x, sep_y, sep_z):
    pieces = [pltpu.VMEM((n, 64, 256), F32) for n in (UP, 8 - UP, 4, 4)]
    hbm = pl.BlockSpec(memory_space=pltpu.HBM)
    sems = [pltpu.SemaphoreType.DMA((4,))]
    made = call(split_kernel, pieces, far(u), far(v), places=[hbm, hbm], scratch_shapes=sems)
    u_up, u_both, v_keep, v_send = made
    v_other = send(v_send, V_SWAP)
    up = send(u_up, U_UP)
    both = send(u_both, U_BOTH)
    other_up = send(u_up, U_CORE)
    other_both = send(u_both, U_CORE)
    v_near = send(v_keep, V_NEXT)
    row = pltpu.VMEM((8, 128), F32)
    outs = (pltpu.VMEM((8, 128), jnp.int32), row, pltpu.VMEM((512, 256), BF16))
    args = (sep_x, sep_y, sep_z, *map(near, (u_up, u_both, v_keep, v_send)), far(w))
    places = [SMEM] * 3 + [VMEM] * 4 + [hbm]
    scratch = [pltpu.VMEM((8, 64, 256), F32), pltpu.SemaphoreType.DMA]
    lags, part, v_parts = map(near, call(own_kernel, outs, *args, places=places, scratch_shapes=scratch))
    outs = (row, pltpu.VMEM((8, 256, 256), BF16))
    part, u_parts = map(near, call(core_kernel, outs, lags, near(u_up), near(u_both), other_up, other_both, part))
    part = call(u_kernel, row, lags, u_parts, up, both, part)
    rows = call(v_kernel, pltpu.VMEM((256, 128), F32), lags, v_parts, v_other, v_near, near(part))
    rows = near(lax.all_to_all(rows, SERVED, 0, 0, tiled=True))
    return call(end_kernel, jax.ShapeDtypeStruct((3, 16), F32), rows)


def solution(mesh):
    finer = Mesh(mesh.devices.reshape(SHAPE), AXES)
    placed = (P(None, GX, GY),) * 3 + (P(),) * 3
    return jax.shard_map(local, mesh=finer, in_specs=placed, out_specs=P(), check_vma=False)
```

```python
import jax
import jax.numpy as jnp
from jax import lax
from jax.experimental import pallas as pl
from jax.experimental.pallas import tpu as pltpu
from jax.sharding import Mesh
from jax.sharding import PartitionSpec as P


SHAPE = (4, 2, 2, 8, 2)
AXES = ("y", "xh", "xl", "z", "c")
SERVED = AXES
GX = ("xl", "z", "c")
GY = ("y", "xh")
F32 = jnp.float32
UP = 3
BF16 = jnp.bfloat16


def pairs_of(target):
    def flat(at):
        index = 0
        for size, i in zip(SHAPE, at):
            index = index * size + i % size
        return index

    places = [()]
    for size in SHAPE:
        places = [at + (i,) for at in places for i in range(size)]
    return [(flat(at), flat(target(*at))) for at in places]


def chip_step(step):
    def target(y, xh, xl, z, c):
        chip = xl * 8 + z + step[c]
        return (y, xh, chip // 8, chip % 8, c)

    return target


U_UP = pairs_of(chip_step((1, 1)))
U_BOTH = pairs_of(chip_step((-1, 1)))
U_CORE = pairs_of(lambda y, xh, xl, z, c: (y, xh, xl, z, 1 - c))
V_SWAP = pairs_of(lambda y, xh, xl, z, c: (y, 1 - xh, xl, z, c))
V_NEXT = pairs_of(lambda y, xh, xl, z, c: (y + (1 if xh else -1), xh, xl, z, c))


def dot_nt(a, b):
    return lax.dot_general(a, b, (((1,), (1,)), ((), ())), preferred_element_type=F32)


def dot_nn(a, b):
    return lax.dot_general(a, b, (((1,), (0,)), ((), ())), preferred_element_type=F32)


def lane_index():
    return lax.broadcasted_iota(jnp.int32, (8, 128), 1)


def row_index():
    return lax.broadcasted_iota(jnp.int32, (8, 128), 0)


def lag_row(refs):
    lane = lane_index()
    lags = jnp.zeros((8, 128), jnp.int32)
    for axis, ref in enumerate(refs):
        for k in range(16):
            lags = jnp.where(lane == axis * 16 + k, ref[k], lags)
    return lags


def skewed(gram):
    rows, lanes = gram.shape
    total = gram[:8]
    for i in range(8, rows, 8):
        total = total + pltpu.roll(gram[i : i + 8], (lanes - i) % lanes, 1)
    return total


def pick(skew, diagonal):
    lanes = skew.shape[1]
    at = (diagonal + row_index()) & (lanes - 1)
    got = jnp.zeros((8, 128), F32)
    for t in range(lanes // 128):
        part = jnp.take_along_axis(skew[:, t * 128 : (t + 1) * 128], at & 127, axis=1)
        got = jnp.where((at >> 7) == t, part, got)
    return jnp.broadcast_to(jnp.sum(got, axis=0, keepdims=True), (8, 128))


def widened(gram):
    return jnp.concatenate([gram, jnp.zeros(gram.shape, F32)], axis=1)


def halves(x):
    high = x.astype(BF16)
    return high, (x - high.astype(F32)).astype(BF16)


def split_kernel(u_ref, v_ref, up, both, keep, swap, sems):
    half = lax.axis_index("xh")
    moves = (
        (v_ref.at[pl.ds(4 - 4 * half, 4)], swap),
        (u_ref.at[pl.ds(0, UP)], up),
        (u_ref.at[pl.ds(UP, 8 - UP)], both),
        (v_ref.at[pl.ds(4 * half, 4)], keep),
    )
    copies = [pltpu.make_async_copy(a, b, sems.at[i]) for i, (a, b) in enumerate(moves)]
    for copy in copies:
        copy.start()
    for copy in copies:
        copy.wait()


def own_kernel(sx, sy, sz, u_up, u_both, keep, swap, w_far, lag_ref, out_ref, v_parts, w_ref, sem):
    fetch = pltpu.make_async_copy(w_far, w_ref, sem)
    fetch.start()
    lags = lag_row((sx, sy, sz))
    lag_ref[...] = lags
    lane = lane_index()
    gram = jnp.zeros((64, 64), F32)
    for piece in (u_up, u_both):
        for z in range(piece.shape[0]):
            high, low = halves(piece[z])
            both = dot_nt(jnp.concatenate([high, low], axis=0), high)
            gram = gram + both[:64] + both[64:] + dot_nt(high, low)
    u_sums = jnp.where(lags < 64, pick(skewed(widened(gram)), lags), 0.0)
    gram = jnp.zeros((256, 256), F32)
    for piece in (keep, swap):
        rows = piece[...].reshape(256, 256)
        high, low = halves(rows)
        t_high, t_low = halves(rows.T)
        gram = gram + dot_nn(t_high, high) + dot_nn(t_low, high) + dot_nn(t_high, low)
        if piece is keep:
            v_parts[:256] = t_high
            v_parts[256:] = t_low
    v_sums = pick(skewed(widened(gram)), lags)
    fetch.wait()
    planes = [w_ref[z] for z in range(8)]
    w_sums = jnp.zeros((8, 128), F32)
    for lag in range(5):
        total = planes[0] * planes[lag]
        for z in range(1, 8 - lag):
            total = total + planes[z] * planes[z + lag]
        total = jnp.sum(jnp.sum(total, axis=0, keepdims=True), axis=1, keepdims=True)
        w_sums = jnp.where(lags == lag, total, w_sums)
    w_sums = w_sums * 8.0 / (8.0 - lags.astype(F32))
    of_u = (lane < 16) | (lane == 48)
    of_v = (lane < 32) | (lane == 49)
    out_ref[...] = jnp.where(of_u, u_sums, jnp.where(of_v, v_sums, w_sums))


def core_kernel(lag_ref, u_up, u_both, other_up, other_both, before, out_ref, u_parts):
    lags = lag_ref[...]
    gram = jnp.zeros((64, 64), F32)
    for z in range(8):
        a_high, a_low = halves(u_up[z] if z < UP else u_both[z - UP])
        b_high, b_low = halves(other_up[z] if z < UP else other_both[z - UP])
        u_parts[z] = jnp.concatenate([b_high, a_high, b_low, a_low], axis=0)
        gram = gram + dot_nt(b_high, a_high) + dot_nt(b_low, a_high) + dot_nt(b_high, a_low)
    counted = (lax.axis_index("c") == 1) & (lane_index() < 16) & (lags < 128)
    out_ref[...] = before[...] + jnp.where(counted, pick(skewed(widened(gram)), lags - 64), 0.0)


def chip_sums(parts, near, planes):
    total = jnp.zeros((128, 64), F32)
    for z in planes:
        high, low = halves(near[z - planes[0]])
        both = dot_nt(parts[z], high)
        total = total + both[:128] + both[128:] + dot_nt(parts[z, :128], low)
    return total


def up_kernel(parts, near_up, out_ref):
    out_ref[...] = chip_sums(parts, near_up, range(UP))


def u_kernel(lag_ref, parts, up_ref, near_both, before, out_ref):
    lags = lag_ref[...]
    first = lax.axis_index("c") == 0
    up = up_ref[...]
    mixed = chip_sums(parts, near_both, range(UP, 8))
    far = jnp.where(first, mixed[64:] + up[64:].T, (mixed[64:] + up[64:]).T)
    next_to = jnp.where(first, mixed[:64], up[:64].T)
    i = lax.broadcasted_iota(jnp.int32, (64, 64), 0)
    j = lax.broadcasted_iota(jnp.int32, (64, 64), 1)
    gram = jnp.concatenate([next_to, jnp.where(j <= i, far, 0.0)], axis=1)
    out_ref[...] = before[...] + jnp.where(lane_index() < 16, pick(skewed(gram), lags - 64), 0.0)


def v_kernel(lag_ref, parts, other, near, before, out_ref):
    lags = lag_ref[...]
    lane = lane_index()
    first = lax.axis_index("xh") == 0
    high, low = halves(other[...].reshape(256, 256))
    near_high, near_low = halves(near[...].reshape(256, 256).T)
    i = lax.broadcasted_iota(jnp.int32, (256, 256), 0)
    j = lax.broadcasted_iota(jnp.int32, (256, 256), 1)
    ahead = jnp.where(first, i - j, j - i)
    sums = jnp.zeros((8, 128), F32)
    for a_high, a_low, sign in ((parts[:256], parts[256:], 1), (near_high, near_low, -1)):
        gram = dot_nn(a_high, high) + dot_nn(a_low, high) + dot_nn(a_high, low)
        gram = jnp.where(ahead * sign >= 0, gram, 0.0)
        sums = sums + pick(skewed(gram), jnp.where(first, lags - 256, 256 - lags) * sign)
    row = before[...] + jnp.where((lane >= 16) & (lane < 32), sums, 0.0)
    for i in range(0, out_ref.shape[0], 8):
        out_ref[i : i + 8] = row


def end_kernel(parts, out_ref):
    total = jnp.sum(parts[...], axis=0, keepdims=True)
    lane = lax.broadcasted_iota(jnp.int32, (1, 128), 1)
    for axis in range(3):
        energy = jnp.sum(jnp.where(lane == 48 + axis, total, 0.0), axis=1, keepdims=True)
        out_ref[axis : axis + 1, :] = total[:, axis * 16 : axis * 16 + 16] / energy


ROOM = {up_kernel: 8, core_kernel: 12, split_kernel: 2, own_kernel: 16, u_kernel: 12, v_kernel: 12, end_kernel: 4}
SMEM = pl.BlockSpec(memory_space=pltpu.SMEM)
VMEM = pl.BlockSpec(memory_space=pltpu.VMEM)


def call(kernel, out, *args, places=None, **more):
    places = places or [SMEM if a.dtype == jnp.int32 and a.ndim == 1 else VMEM for a in args]
    specs = jax.tree.map(lambda _: VMEM, out)
    room = pltpu.CompilerParams(vmem_limit_bytes=ROOM[kernel] * 2**20)
    return pl.pallas_call(kernel, out_shape=out, in_specs=places, out_specs=specs, compiler_params=room, **more)(*args)


def near(x):
    return pltpu.with_memory_space_constraint(x, pltpu.VMEM)


def far(x):
    return pltpu.with_memory_space_constraint(x, pltpu.HBM)


def send(value, pairs):
    return near(lax.ppermute(value, AXES, pairs))


def local(u, v, w, sep_x, sep_y, sep_z):
    pieces = [pltpu.VMEM((n, 64, 256), F32) for n in (UP, 8 - UP, 4, 4)]
    hbm = pl.BlockSpec(memory_space=pltpu.HBM)
    sems = [pltpu.SemaphoreType.DMA((4,))]
    made = call(split_kernel, pieces, far(u), far(v), places=[hbm, hbm], scratch_shapes=sems)
    u_up, u_both, v_keep, v_send = made
    v_other = send(v_send, V_SWAP)
    up = send(u_up, U_UP)
    both = send(u_both, U_BOTH)
    other_up = send(u_up, U_CORE)
    other_both = send(u_both, U_CORE)
    v_near = send(v_keep, V_NEXT)
    row = pltpu.VMEM((8, 128), F32)
    outs = (pltpu.VMEM((8, 128), jnp.int32), row, pltpu.VMEM((512, 256), BF16))
    args = (sep_x, sep_y, sep_z, *map(near, (u_up, u_both, v_keep, v_send)), far(w))
    places = [SMEM] * 3 + [VMEM] * 4 + [hbm]
    scratch = [pltpu.VMEM((8, 64, 256), F32), pltpu.SemaphoreType.DMA]
    lags, part, v_parts = map(near, call(own_kernel, outs, *args, places=places, scratch_shapes=scratch))
    outs = (row, pltpu.VMEM((8, 256, 256), BF16))
    part, u_parts = map(near, call(core_kernel, outs, lags, near(u_up), near(u_both), other_up, other_both, part))
    early = call(up_kernel, pltpu.VMEM((128, 64), F32), u_parts, up)
    part = call(u_kernel, row, lags, u_parts, near(early), both, part)
    rows = call(v_kernel, pltpu.VMEM((256, 128), F32), lags, v_parts, v_other, v_near, near(part))
    rows = near(lax.all_to_all(rows, SERVED, 0, 0, tiled=True))
    return call(end_kernel, jax.ShapeDtypeStruct((3, 16), F32), rows)


def solution(mesh):
    finer = Mesh(mesh.devices.reshape(SHAPE), AXES)
    placed = (P(None, GX, GY),) * 3 + (P(),) * 3
    return jax.shard_map(local, mesh=finer, in_specs=placed, out_specs=P(), check_vma=False)
```

```python
import jax
import jax.numpy as jnp
from jax import lax
from jax.experimental import pallas as pl
from jax.experimental.pallas import tpu as pltpu
from jax.sharding import Mesh
from jax.sharding import PartitionSpec as P


SHAPE = (4, 2, 2, 8, 2)
AXES = ("y", "xh", "xl", "z", "c")
SERVED = AXES
GX = ("xl", "z", "c")
GY = ("y", "xh")
F32 = jnp.float32
UP = 3
BF16 = jnp.bfloat16


def pairs_of(target):
    def flat(at):
        index = 0
        for size, i in zip(SHAPE, at):
            index = index * size + i % size
        return index

    places = [()]
    for size in SHAPE:
        places = [at + (i,) for at in places for i in range(size)]
    return [(flat(at), flat(target(*at))) for at in places]


def chip_step(step):
    def target(y, xh, xl, z, c):
        chip = xl * 8 + z + step[c]
        return (y, xh, chip // 8, chip % 8, c)

    return target


U_UP = pairs_of(chip_step((1, 1)))
U_BOTH = pairs_of(chip_step((-1, 1)))
U_CORE = pairs_of(lambda y, xh, xl, z, c: (y, xh, xl, z, 1 - c))
V_SWAP = pairs_of(lambda y, xh, xl, z, c: (y, 1 - xh, xl, z, c))
V_NEXT = pairs_of(lambda y, xh, xl, z, c: (y + (1 if xh else -1), xh, xl, z, c))


def dot_nt(a, b):
    return lax.dot_general(a, b, (((1,), (1,)), ((), ())), preferred_element_type=F32)


def dot_nn(a, b):
    return lax.dot_general(a, b, (((1,), (0,)), ((), ())), preferred_element_type=F32)


def lane_index():
    return lax.broadcasted_iota(jnp.int32, (8, 128), 1)


def row_index():
    return lax.broadcasted_iota(jnp.int32, (8, 128), 0)


def lag_row(refs):
    lane = lane_index()
    lags = jnp.zeros((8, 128), jnp.int32)
    for axis, ref in enumerate(refs):
        for k in range(16):
            lags = jnp.where(lane == axis * 16 + k, ref[k], lags)
    return lags


def skewed(gram):
    rows, lanes = gram.shape
    total = gram[:8]
    for i in range(8, rows, 8):
        total = total + pltpu.roll(gram[i : i + 8], (lanes - i) % lanes, 1)
    return total


def pick(skew, diagonal):
    lanes = skew.shape[1]
    at = (diagonal + row_index()) & (lanes - 1)
    got = jnp.zeros((8, 128), F32)
    for t in range(lanes // 128):
        part = jnp.take_along_axis(skew[:, t * 128 : (t + 1) * 128], at & 127, axis=1)
        got = jnp.where((at >> 7) == t, part, got)
    return jnp.broadcast_to(jnp.sum(got, axis=0, keepdims=True), (8, 128))


def widened(gram):
    return jnp.concatenate([gram, jnp.zeros(gram.shape, F32)], axis=1)


def halves(x):
    high = x.astype(BF16)
    return high, (x - high.astype(F32)).astype(BF16)


def split_kernel(u_ref, v_ref, up, both, keep, swap, sems):
    half = lax.axis_index("xh")
    moves = (
        (v_ref.at[pl.ds(4 - 4 * half, 4)], swap),
        (u_ref.at[pl.ds(0, UP)], up),
        (u_ref.at[pl.ds(UP, 8 - UP)], both),
        (v_ref.at[pl.ds(4 * half, 4)], keep),
    )
    copies = [pltpu.make_async_copy(a, b, sems.at[i]) for i, (a, b) in enumerate(moves)]
    for copy in copies:
        copy.start()
    for copy in copies:
        copy.wait()


def own_kernel(sx, sy, sz, u_up, u_both, keep, swap, w_far, lag_ref, out_ref, v_parts, w_ref, sem):
    fetch = pltpu.make_async_copy(w_far, w_ref, sem)
    fetch.start()
    lags = lag_row((sx, sy, sz))
    lag_ref[...] = lags
    lane = lane_index()
    gram = jnp.zeros((64, 64), F32)
    for piece in (u_up, u_both):
        for z in range(piece.shape[0]):
            high, low = halves(piece[z])
            both = dot_nt(jnp.concatenate([high, low], axis=0), high)
            gram = gram + both[:64] + both[64:] + dot_nt(high, low)
    u_sums = jnp.where(lags < 64, pick(skewed(widened(gram)), lags), 0.0)
    gram = jnp.zeros((256, 256), F32)
    for piece in (keep, swap):
        rows = piece[...].reshape(256, 256)
        high, low = halves(rows)
        t_high, t_low = halves(rows.T)
        gram = gram + dot_nn(t_high, high) + dot_nn(t_low, high) + dot_nn(t_high, low)
        if piece is keep:
            v_parts[:256] = t_high
            v_parts[256:] = t_low
    v_sums = pick(skewed(widened(gram)), lags)
    fetch.wait()
    planes = [w_ref[z] for z in range(8)]
    w_sums = jnp.zeros((8, 128), F32)
    for lag in range(5):
        total = planes[0] * planes[lag]
        for z in range(1, 8 - lag):
            total = total + planes[z] * planes[z + lag]
        total = jnp.sum(jnp.sum(total, axis=0, keepdims=True), axis=1, keepdims=True)
        w_sums = jnp.where(lags == lag, total, w_sums)
    w_sums = w_sums * 8.0 / (8.0 - lags.astype(F32))
    of_u = (lane < 16) | (lane == 48)
    of_v = (lane < 32) | (lane == 49)
    out_ref[...] = jnp.where(of_u, u_sums, jnp.where(of_v, v_sums, w_sums))


def core_kernel(lag_ref, u_up, u_both, other_up, other_both, before, out_ref, u_parts):
    lags = lag_ref[...]
    gram = jnp.zeros((64, 64), F32)
    for z in range(8):
        a_high, a_low = halves(u_up[z] if z < UP else u_both[z - UP])
        b_high, b_low = halves(other_up[z] if z < UP else other_both[z - UP])
        u_parts[z] = jnp.concatenate([b_high, a_high, b_low, a_low], axis=0)
        gram = gram + dot_nt(b_high, a_high) + dot_nt(b_low, a_high) + dot_nt(b_high, a_low)
    counted = (lax.axis_index("c") == 1) & (lane_index() < 16) & (lags < 128)
    out_ref[...] = before[...] + jnp.where(counted, pick(skewed(widened(gram)), lags - 64), 0.0)


def chip_sums(parts, near, planes):
    total = jnp.zeros((128, 64), F32)
    for z in planes:
        high, low = halves(near[z - planes[0]])
        both = dot_nt(parts[z], high)
        total = total + both[:128] + both[128:] + dot_nt(parts[z, :128], low)
    return total


def up_kernel(parts, near_up, out_ref):
    out_ref[...] = chip_sums(parts, near_up, range(UP)).T


def u_kernel(lag_ref, parts, up_ref, near_both, before, out_ref):
    lags = lag_ref[...]
    first = lax.axis_index("c") == 0
    up = up_ref[...]
    mixed = chip_sums(parts, near_both, range(UP, 8))
    far = jnp.where(first, mixed[64:], mixed[64:].T) + up[:, 64:]
    next_to = jnp.where(first, mixed[:64], up[:, :64])
    i = lax.broadcasted_iota(jnp.int32, (64, 64), 0)
    j = lax.broadcasted_iota(jnp.int32, (64, 64), 1)
    gram = jnp.concatenate([next_to, jnp.where(j <= i, far, 0.0)], axis=1)
    out_ref[...] = before[...] + jnp.where(lane_index() < 16, pick(skewed(gram), lags - 64), 0.0)


def v_kernel(lag_ref, parts, other, near, before, out_ref):
    lags = lag_ref[...]
    lane = lane_index()
    first = lax.axis_index("xh") == 0
    high, low = halves(other[...].reshape(256, 256))
    near_high, near_low = halves(near[...].reshape(256, 256).T)
    i = lax.broadcasted_iota(jnp.int32, (256, 256), 0)
    j = lax.broadcasted_iota(jnp.int32, (256, 256), 1)
    ahead = jnp.where(first, i - j, j - i)
    sums = jnp.zeros((8, 128), F32)
    for a_high, a_low, sign in ((parts[:256], parts[256:], 1), (near_high, near_low, -1)):
        gram = dot_nn(a_high, high) + dot_nn(a_low, high) + dot_nn(a_high, low)
        gram = jnp.where(ahead * sign >= 0, gram, 0.0)
        sums = sums + pick(skewed(gram), jnp.where(first, lags - 256, 256 - lags) * sign)
    row = before[...] + jnp.where((lane >= 16) & (lane < 32), sums, 0.0)
    for i in range(0, out_ref.shape[0], 8):
        out_ref[i : i + 8] = row


def end_kernel(parts, out_ref):
    total = jnp.sum(parts[...], axis=0, keepdims=True)
    lane = lax.broadcasted_iota(jnp.int32, (1, 128), 1)
    for axis in range(3):
        energy = jnp.sum(jnp.where(lane == 48 + axis, total, 0.0), axis=1, keepdims=True)
        out_ref[axis : axis + 1, :] = total[:, axis * 16 : axis * 16 + 16] / energy


ROOM = {up_kernel: 8, core_kernel: 12, split_kernel: 2, own_kernel: 16, u_kernel: 12, v_kernel: 12, end_kernel: 4}
SMEM = pl.BlockSpec(memory_space=pltpu.SMEM)
VMEM = pl.BlockSpec(memory_space=pltpu.VMEM)


def call(kernel, out, *args, places=None, **more):
    places = places or [SMEM if a.dtype == jnp.int32 and a.ndim == 1 else VMEM for a in args]
    specs = jax.tree.map(lambda _: VMEM, out)
    room = pltpu.CompilerParams(vmem_limit_bytes=ROOM[kernel] * 2**20)
    return pl.pallas_call(kernel, out_shape=out, in_specs=places, out_specs=specs, compiler_params=room, **more)(*args)


def near(x):
    return pltpu.with_memory_space_constraint(x, pltpu.VMEM)


def far(x):
    return pltpu.with_memory_space_constraint(x, pltpu.HBM)


def send(value, pairs):
    return near(lax.ppermute(value, AXES, pairs))


def local(u, v, w, sep_x, sep_y, sep_z):
    pieces = [pltpu.VMEM((n, 64, 256), F32) for n in (UP, 8 - UP, 4, 4)]
    hbm = pl.BlockSpec(memory_space=pltpu.HBM)
    sems = [pltpu.SemaphoreType.DMA((4,))]
    made = call(split_kernel, pieces, far(u), far(v), places=[hbm, hbm], scratch_shapes=sems)
    u_up, u_both, v_keep, v_send = made
    v_other = send(v_send, V_SWAP)
    up = send(u_up, U_UP)
    both = send(u_both, U_BOTH)
    other_up = send(u_up, U_CORE)
    other_both = send(u_both, U_CORE)
    v_near = send(v_keep, V_NEXT)
    row = pltpu.VMEM((8, 128), F32)
    outs = (pltpu.VMEM((8, 128), jnp.int32), row, pltpu.VMEM((512, 256), BF16))
    args = (sep_x, sep_y, sep_z, *map(near, (u_up, u_both, v_keep, v_send)), far(w))
    places = [SMEM] * 3 + [VMEM] * 4 + [hbm]
    scratch = [pltpu.VMEM((8, 64, 256), F32), pltpu.SemaphoreType.DMA]
    lags, part, v_parts = map(near, call(own_kernel, outs, *args, places=places, scratch_shapes=scratch))
    outs = (row, pltpu.VMEM((8, 256, 256), BF16))
    part, u_parts = map(near, call(core_kernel, outs, lags, near(u_up), near(u_both), other_up, other_both, part))
    early = call(up_kernel, pltpu.VMEM((64, 128), F32), u_parts, up)
    part = call(u_kernel, row, lags, u_parts, near(early), both, part)
    rows = call(v_kernel, pltpu.VMEM((256, 128), F32), lags, v_parts, v_other, v_near, near(part))
    rows = near(lax.all_to_all(rows, SERVED, 0, 0, tiled=True))
    return call(end_kernel, jax.ShapeDtypeStruct((3, 16), F32), rows)


def solution(mesh):
    finer = Mesh(mesh.devices.reshape(SHAPE), AXES)
    placed = (P(None, GX, GY),) * 3 + (P(),) * 3
    return jax.shard_map(local, mesh=finer, in_specs=placed, out_specs=P(), check_vma=False)
```
